16 devices in a mesh: rep: 4 (over y, z, core), dp: 4 (over x).
Axes of the slice: x: 4, y: 2, z: 1, core: 2. Of those that a mesh axis runs over, the one named last changes fastest.
The devices are a block of a 4x4x8 slice.
Arguments:
- x: bfloat16 [16, 2048, 896], P(('rep', 'dp')), parts along dimension 0
- dy: bfloat16 [16, 2048, 896], P(('rep', 'dp')), parts along dimension 0
- w_gate: bfloat16 [2, 896, 4864], P(None, 'dp')
- w_up: bfloat16 [2, 896, 4864], P(None, 'dp')
- w_down: bfloat16 [2, 4864, 896], P(None, 'dp')
- m_w_gate: float32 [2, 896, 4864], P(None, 'dp')
- m_w_up: float32 [2, 896, 4864], P(None, 'dp')
- m_w_down: float32 [2, 4864, 896], P(None, 'dp')
- v_w_gate: float32 [2, 896, 4864], P(None, 'dp')
- v_w_up: float32 [2, 896, 4864], P(None, 'dp')
- v_w_down: float32 [2, 4864, 896], P(None, 'dp')
Outputs:
- output 1: bfloat16 [8, 896, 4864], P('rep', 'dp'), parts along dimension 0
- output 2: bfloat16 [8, 896, 4864], P('rep', 'dp'), parts along dimension 0
- output 3: bfloat16 [8, 4864, 896], P('rep', 'dp'), parts along dimension 0
- output 4: float32 [8, 896, 4864], P('rep', 'dp'), parts along dimension 0
- output 5: float32 [8, 896, 4864], P('rep', 'dp'), parts along dimension 0
- output 6: float32 [8, 4864, 896], P('rep', 'dp'), parts along dimension 0
- output 7: float32 [8, 896, 4864], P('rep', 'dp'), parts along dimension 0
- output 8: float32 [8, 896, 4864], P('rep', 'dp'), parts along dimension 0
- output 9: float32 [8, 4864, 896], P('rep', 'dp'), parts along dimension 0
There are 4 independent parts. The reference program is written for one: setup_inputs(seed, part) draws one part's arguments, and reference() takes and returns one part's arrays. A program takes and returns all parts, laid end to end along the dimension named above; an argument that names none is the same for every part.
All inputs are finite; a program needn't handle non-finite values.
Results may differ from the reference program's by a relative error of at most 0.022.
Values are sent between devices in bfloat16 or wider.
A program may use at most 768 MiB of HBM per device.

```python
import jax
import jax.numpy as jnp
from jax import lax

SEQUENCES = 4
TOKENS = 2048
D = 896
FF = 4864
LAYERS = 2
NAMES = ("w_gate", "w_up", "w_down")
SHAPES = {"w_gate": (LAYERS, D, FF), "w_up": (LAYERS, D, FF), "w_down": (LAYERS, FF, D)}


def bump(key, n, height):
    away = (jnp.arange(n, dtype=jnp.int32) - jax.random.randint(key, (), 0, n, jnp.int32)) % n
    return jnp.where(away < n // 8, height, 1.0)


def together(key, own, strength):
    shared = jax.random.normal(key, own.shape[1:], jnp.float32)
    return (own + strength * shared) * lax.rsqrt(1 + strength * strength)


def setup_inputs(seed: int = 0, part: int = 0) -> dict:
    kx, kdy, ka, kb, kz, kf, kh, kl, *keys = jax.random.split(jax.random.key(seed), 8 + 3 * len(NAMES))
    kx, kdy, ka, kb = (jax.random.fold_in(k, part) for k in (kx, kdy, ka, kb))
    kw, km, kv = (keys[i::3] for i in range(3))
    shape = (SEQUENCES, TOKENS, D)
    much_x, much_dy = jax.random.uniform(kz, (2,), jnp.float32, 0.0, 1.0)
    loud = 2.0 ** jax.random.uniform(jax.random.fold_in(kz, 1), (), jnp.float32, -1.0, 2.0)
    layers = 2.0 ** jax.random.uniform(kl, (LAYERS, 1, 1), jnp.float32, -1.0, 1.0)
    x = together(ka, jax.random.normal(kx, shape, jnp.float32), much_x) * bump(kf, D, 4.0)
    dy = together(kb, jax.random.normal(kdy, shape, jnp.float32), much_dy)
    drawn = {"x": x.astype(jnp.bfloat16), "dy": (loud * dy * (SEQUENCES * TOKENS) ** -0.5).astype(jnp.bfloat16)}
    for key, name in zip(kw, NAMES, strict=True):
        w = jax.random.normal(key, SHAPES[name], jnp.float32) * SHAPES[name][1] ** -0.5
        drawn[name] = (w * {"w_gate": 1.0, "w_up": bump(kh, FF, 4.0), "w_down": layers}[name]).astype(jnp.bfloat16)
    for key, name in zip(km, NAMES, strict=True):
        drawn[f"m_{name}"] = 0.1 * jax.random.normal(key, SHAPES[name], jnp.float32)
    for key, name in zip(kv, NAMES, strict=True):
        drawn[f"v_{name}"] = jax.random.uniform(key, SHAPES[name], jnp.float32, 0.005, 0.015)
    return drawn


def matmul(a, w):
    return jnp.dot(a, w, preferred_element_type=jnp.float32).astype(jnp.bfloat16)


def normed(h):
    wide = h.astype(jnp.float32)
    scale = lax.rsqrt(jnp.mean(wide**2, -1, keepdims=True) + 1e-6)
    return (wide * scale).astype(jnp.bfloat16)


def layer(h, w):
    a = normed(h)
    gate = jnp.dot(a, w["w_gate"], preferred_element_type=jnp.float32)
    up = jnp.dot(a, w["w_up"], preferred_element_type=jnp.float32)
    return h + matmul((jax.nn.silu(gate) * up).astype(jnp.bfloat16), w["w_down"])


def adamw(w, m, v, g):
    m = 0.9 * m + 0.1 * g
    v = 0.95 * v + 0.05 * g * g
    step = m * lax.rsqrt(v + 1e-8) + 0.1 * w
    return (w - 0.02 * step).astype(jnp.bfloat16), m, v


def clipped(gradients, sum_of_squares, count):
    factor = jnp.minimum(1.0, 0.5 * lax.rsqrt(sum_of_squares / count + 1e-30))
    return [g * factor for g in gradients]


def stack(weights, h):
    return lax.scan(lambda h, w: (layer(h, w), None), h, weights)[0]


def reference(x, dy, w_gate, w_up, w_down, m_w_gate, m_w_up, m_w_down, v_w_gate, v_w_up, v_w_down):
    weights = dict(zip(NAMES, (w_gate, w_up, w_down), strict=True))

    def take(so_far, sequence):
        h, by_y = sequence
        _, back = jax.vjp(lambda w: stack(w, h), weights)
        return jax.tree.map(lambda total, term: total + term.astype(jnp.float32), so_far, back(by_y)[0]), None

    none_yet = {name: jnp.zeros(w.shape, jnp.float32) for name, w in weights.items()}
    by_weights, _ = lax.scan(take, none_yet, (x, dy))
    gradients = [by_weights[name].astype(jnp.bfloat16).astype(jnp.float32) for name in NAMES]
    gradients = clipped(gradients, sum(jnp.sum(g * g) for g in gradients), sum(g.size for g in gradients))
    new = [
        adamw(w.astype(jnp.float32), m, v, g)
        for w, m, v, g in zip((w_gate, w_up, w_down), (m_w_gate, m_w_up, m_w_down), (v_w_gate, v_w_up, v_w_down), gradients, strict=True)
    ]
    return tuple(one[which] for which in range(3) for one in new)
```

```python
import jax
import jax.numpy as jnp
from jax import lax
from jax.experimental import pallas as pl
from jax.experimental.pallas import tpu as pltpu
from jax.sharding import PartitionSpec as P

F32, BF16 = jnp.float32, jnp.bfloat16
TILE = 256
RING = 8
KEEP = 4


def nn(a, b):
    return lax.dot_general(a, b, (((1,), (0,)), ((), ())), preferred_element_type=F32)


def nt(a, b):
    return lax.dot_general(a, b, (((1,), (1,)), ((), ())), preferred_element_type=F32)


def tn(a, b):
    return lax.dot_general(a, b, (((0,), (0,)), ((), ())), preferred_element_type=F32)


def exchange(n, tokens, d, ff, layers):
    assert n == 4 and layers == 2
    dl, fl, nt_ = d // n, ff // n, ff // TILE
    half, piece = dl // 2, fl // nt_ // 2
    quarter = piece // 2
    rows = min(512, tokens)
    NT = nt_

    def body(
        x, dy, wg, wu, wd,
        gg, gu, gd, stat, WGU, WD, DWD,
        a, aT, y, yT, h, acc, prod, dgu, wgu_v, wd_v, dw, dwd, fg, fd, og, od, own,
        l1l, l1r, l2l, l2r, l3l, l3r, k1l, k1r, k2l, k2r, k3l, k3r, sg, sd, st,
        ad_s, ad_r, ag_s, ag_r, rg_s, rg_r, rd_s, rd_r, ld, lown, lout, lst, lin, st_s, st_r,
    ):
        me, rep = lax.axis_index("dp"), lax.axis_index("rep")
        right, left, far = (lax.rem(me + k, n) for k in (1, n - 1, 2))
        core = lax.rem(rep, 2)
        R, L, O, C = {"dp": right}, {"dp": left}, {"dp": far}, {"rep": rep + 1 - 2 * core}

        def remote(src, dst, ss, rs, to):
            return lambda: pltpu.make_async_remote_copy(
                src_ref=src, dst_ref=dst, send_sem=ss, recv_sem=rs, device_id=to, device_id_type=pl.DeviceIdType.MESH
            )

        def local(src, dst, sem):
            return lambda: pltpu.make_async_copy(src, dst, sem)

        def ds(at, size, by=16):
            return pl.ds(pl.multiple_of(at, by), size)

        barrier = pltpu.get_barrier_semaphore()
        for to in (R, L, O, C):
            pl.semaphore_signal(barrier, inc=1, device_id=to, device_id_type=pl.DeviceIdType.MESH)
        pl.semaphore_wait(barrier, 4)

        def d_rows(block, j):
            return block * fl + core * (fl // 2) + j * piece

        def d_first(v):
            l, j, s = lax.div(v, NT), lax.rem(v, NT), lax.rem(v, RING)
            src, dst = wd.at[l, ds(core * (fl // 2) + j * piece, piece)], WD.at[l, ds(d_rows(me, j), piece)]
            return [remote(src, dst, ad_s.at[0, s], ad_r.at[0, s], R), remote(src, dst, ad_s.at[1, s], ad_r.at[1, s], L)]

        def d_next(v):
            l, j, s = lax.div(v, NT), lax.rem(v, NT), lax.rem(v, RING)
            lo, hi = WD.at[l, ds(d_rows(left, j), quarter)], WD.at[l, ds(d_rows(right, j) + quarter, quarter)]
            pa, pb = WD.at[l, ds(d_rows(left, j), piece)], WD.at[l, ds(d_rows(right, j), piece)]
            return [
                remote(lo, lo, ad_s.at[2, s], ad_r.at[2, s], R),
                remote(hi, hi, ad_s.at[3, s], ad_r.at[3, s], L),
                remote(pa, pa, ad_s.at[4, s], ad_r.at[4, s], C),
                remote(pb, pb, ad_s.at[5, s], ad_r.at[5, s], C),
            ]

        def d_far(v):
            l, j, s = lax.div(v, NT), lax.rem(v, NT), lax.rem(v, RING)
            pc = WD.at[l, ds(d_rows(far, j), piece)]
            return [remote(pc, pc, ad_s.at[6, s], ad_r.at[6, s], C)]

        def g_rows(block):
            return ds(block * dl + core * half, half)

        def g_first(u):
            l, j, s = lax.div(u, NT), lax.rem(u, NT), lax.rem(u, RING)
            out = []
            for k, w in enumerate((wg, wu)):
                src = w.at[l, ds(core * half, half), ds(j * TILE, TILE, TILE)]
                dst = WGU.at[l, j, g_rows(me), pl.ds(k * TILE, TILE)]
                out += [
                    remote(src, dst, ag_s.at[k, s], ag_r.at[k, s], R),
                    remote(src, dst, ag_s.at[2 + k, s], ag_r.at[2 + k, s], L),
                ]
            return out

        def g_next(u):
            l, j, s = lax.div(u, NT), lax.rem(u, NT), lax.rem(u, RING)
            lo, hi = WGU.at[l, j, g_rows(left), pl.ds(0, TILE)], WGU.at[l, j, g_rows(right), pl.ds(TILE, TILE)]
            pa, pb = WGU.at[l, j, g_rows(left)], WGU.at[l, j, g_rows(right)]
            return [
                remote(lo, lo, ag_s.at[4, s], ag_r.at[4, s], R),
                remote(hi, hi, ag_s.at[5, s], ag_r.at[5, s], L),
                remote(pa, pa, ag_s.at[6, s], ag_r.at[6, s], C),
                remote(pb, pb, ag_s.at[7, s], ag_r.at[7, s], C),
            ]

        def g_far(u):
            l, j, s = lax.div(u, NT), lax.rem(u, NT), lax.rem(u, RING)
            pc = WGU.at[l, j, g_rows(far)]
            return [remote(pc, pc, ag_s.at[8, s], ag_r.at[8, s], C)]

        def loads(l, j):
            s = lax.rem(j, 2)
            out = [
                local(wg.at[l, :, ds(j * TILE, TILE, TILE)], wgu_v.at[s, ds(me * dl, dl), pl.ds(0, TILE)], ld.at[0, s]),
                local(wu.at[l, :, ds(j * TILE, TILE, TILE)], wgu_v.at[s, ds(me * dl, dl), pl.ds(TILE, TILE)], ld.at[1, s]),
                local(WD.at[l, ds(j * TILE, TILE)], wd_v.at[s], ld.at[2, s]),
            ]
            for k, block in enumerate((right, left, far)):
                at = ds(block * dl, dl)
                out.append(local(WGU.at[l, j, at], wgu_v.at[s, at], ld.at[3 + k, s]))
            return out

        def sum_first(src, slot, land, ss, rs, size):
            return [
                remote(src(far, 0), land[0].at[slot], ss.at[0, slot], rs.at[0, slot], R),
                remote(src(far, 1), land[1].at[slot], ss.at[1, slot], rs.at[1, slot], L),
                remote(src(right, 1), land[2].at[slot], ss.at[2, slot], rs.at[2, slot], R),
                remote(src(left, 0), land[3].at[slot], ss.at[3, slot], rs.at[3, slot], L),
            ]

        def sum_next(out, slot, land, ss, rs):
            return [
                remote(out.at[lax.rem(slot, KEEP), 0], land[4].at[slot], ss.at[4, slot], rs.at[4, slot], R),
                remote(out.at[lax.rem(slot, KEEP), 1], land[5].at[slot], ss.at[5, slot], rs.at[5, slot], L),
            ]

        land_g, land_d = (l1l, l1r, l2l, l2r, l3l, l3r), (k1l, k1r, k2l, k2r, k3l, k3r)

        def rg_first(u):
            q = lax.rem(u, KEEP)
            return sum_first(lambda b, k: dw.at[q, ds(b * dl + k * half, half)], lax.rem(u, RING), land_g, rg_s, rg_r, half)

        def rg_next(u):
            return sum_next(og, lax.rem(u, RING), land_g, rg_s, rg_r)

        def rd_first(v):
            l, j = 1 - lax.div(v, NT), lax.rem(v, NT)
            at = lambda b, k: DWD.at[l, ds(b * fl + (2 * j + k) * piece, piece)]
            return sum_first(at, lax.rem(v, RING), land_d, rd_s, rd_r, piece)

        def rd_next(v):
            return sum_next(od, lax.rem(v, RING), land_d, rd_s, rd_r)

        def own_loads(v):
            l, j, s = 1 - lax.div(v, NT), lax.rem(v, NT), lax.rem(v, RING)
            at = lambda b, k, m: DWD.at[l, ds(b * fl + (2 * j + k) * piece, m * piece)]
            return [
                local(at(right, 0, 1), own.at[s, pl.ds(0, piece)], lown.at[0, s]),
                local(at(left, 1, 1), own.at[s, pl.ds(piece, piece)], lown.at[1, s]),
                local(at(me, 0, 2), own.at[s, pl.ds(2 * piece, 2 * piece)], lown.at[2, s]),
            ]

        def g_out(u):
            l, j, s = 1 - lax.div(u, NT), lax.rem(u, NT), lax.rem(u, 2)
            to = ds(j * TILE, TILE, TILE)
            return [
                local(fg.at[s, :, pl.ds(0, TILE)], gg.at[l, :, to], lout.at[0, s]),
                local(fg.at[s, :, pl.ds(TILE, TILE)], gu.at[l, :, to], lout.at[1, s]),
            ]

        def d_out(v):
            l, j, s = 1 - lax.div(v, NT), lax.rem(v, NT), lax.rem(v, 2)
            return [local(fd.at[s], gd.at[l, ds(j * 2 * piece, 2 * piece)], lout.at[2, s])]

        def dwd_out(u):
            l, j, s = 1 - lax.div(u, NT), lax.rem(u, NT), lax.rem(u, 2)
            return [local(dwd.at[s], DWD.at[l, ds(j * TILE, TILE)], lst.at[s])]

        def start(copies):
            for c in copies:
                c().start()

        def arrived(copies):
            for c in copies:
                c().wait_recv()

        def sent(copies):
            for c in copies:
                c().wait_send()

        def done(copies):
            for c in copies:
                c().wait()

        def wide(ref):
            return ref.astype(F32)

        tF = NT + 8
        tL, tB, tE = tF + NT, tF + 2 * NT, tF + 3 * NT
        end = tE + NT + 5
        blk = min(256, tokens)
        nblk = tokens // blk

        own_w = [local(wd.at[l], buf, lin.at[l]) for l, buf in ((0, y.at[pl.ds(0, fl)]), (1, h.at[pl.ds(0, fl)]))]
        put_w = [local(buf, WD.at[l, ds(me * fl, fl)], lin.at[l]) for l, buf in ((0, y.at[pl.ds(0, fl)]), (1, h.at[pl.ds(0, fl)]))]
        own_x = [local(x, h, lin.at[2]), local(dy, y, lin.at[3])]

        def norm_into(l, r):
            hw = wide(h[r, :])
            scale = lax.rsqrt(jnp.mean(hw * hw, -1, keepdims=True) + 1e-6)
            n_ = (hw * scale).astype(BF16)
            a[l, r, :] = n_
            aT[l, :, r] = n_.T

        def loop(t, _):
            def at(t0, count, f):
                k = t - t0

                @pl.when((k >= 0) & (k < count))
                def _():
                    f(k)

            at(8, 2 * NT, lambda v: sent(d_first(v) + d_next(v) + d_far(v)))
            at(tF + 1, 2 * NT, lambda u: sent(g_first(u) + g_next(u) + g_far(u)))
            at(0, 2 * NT, lambda v: start(d_first(v)))
            at(tF - 4, 2 * NT, lambda u: start(g_first(u)))
            at(tL + 1, 2 * NT, lambda u: start(rg_first(u)))
            at(tB + 1, 2 * NT, lambda v: start(rd_first(v) + own_loads(v)))

            @pl.when(t == 0)
            def _():
                start(own_w)

            @pl.when(t == 1)
            def _():
                done(own_w)
                start(put_w)

            @pl.when(t == 2)
            def _():
                done(put_w)
                start(own_x)
                acc[...] = jnp.zeros_like(acc)
                sg[...] = jnp.zeros_like(sg)
                sd[...] = jnp.zeros_like(sd)

            @pl.when(t == 3)
            def _():
                done(own_x)

            def begin(m):
                r = ds(m * blk, blk, blk)
                norm_into(0, r)
                yT[:, r] = y[r, :].T

            at(4, nblk, begin)

            def d_pass(v):
                arrived(d_first(v))
                start(d_next(v))

            def d_last(v):
                arrived(d_next(v)[:2])
                start(d_far(v))

            at(3, 2 * NT, d_pass)
            at(6, 2 * NT, d_last)
            at(7, 2 * NT, lambda v: arrived(d_next(v)[2:] + d_far(v)))

            @pl.when(t == tL)
            def _():
                def piece_(m, _):
                    r = ds(m * blk, blk, blk)
                    h[r, :] = (wide(h[r, :]) + wide(acc[r, :].astype(BF16))).astype(BF16)
                    acc[r, :] = jnp.zeros((blk, d), F32)
                    norm_into(1, r)
                    return 0

                lax.fori_loop(0, nblk, piece_, 0)

            @pl.when(t == tB)
            def _():
                def piece_(m, _):
                    r = ds(m * blk, blk, blk)
                    hw, da = wide(h[r, :]), wide(acc[r, :].astype(BF16))
                    scale = lax.rsqrt(jnp.mean(hw * hw, -1, keepdims=True) + 1e-6)
                    by_scale = jnp.sum(da * hw, -1, keepdims=True)
                    by_h = (da * scale - hw * (by_scale * scale * scale * scale * (1.0 / d))).astype(BF16)
                    by = (wide(y[r, :]) + wide(by_h)).astype(BF16)
                    y[r, :] = by
                    yT[:, r] = by.T
                    return 0

                lax.fori_loop(0, nblk, piece_, 0)

            def forward(j):
                s = lax.rem(j, 2)
                done(loads(0, j))

                def part(m, _):
                    r = ds(m * rows, rows, rows)
                    both = nn(a[0, r, :], wgu_v[s])
                    gate, up = both[:, :TILE], both[:, TILE:]
                    p = (gate * (1 / (1 + jnp.exp(-gate))) * up).astype(BF16)
                    acc[r, :] += nn(p, wd_v[s])
                    return 0

                lax.fori_loop(0, tokens // rows, part, 0)

            at(tF, NT, forward)

            def back_1(u):
                l, s = 1 - lax.div(u, NT), lax.rem(lax.rem(u, NT), 2)
                done(loads(l, lax.rem(u, NT)))

                def part(m, _):
                    r = ds(m * rows, rows, rows)
                    both = nn(a[l, r, :], wgu_v[s])
                    gate, up = both[:, :TILE], both[:, TILE:]
                    by = wide(nt(y[r, :], wd_v[s]).astype(BF16))
                    sig = 1 / (1 + jnp.exp(-gate))
                    act = gate * sig
                    prod[r, :] = (act * up).astype(BF16)
                    dgu[r, TILE:] = (by * act).astype(BF16)
                    dgu[r, :TILE] = (by * up * (sig * (1 + gate * (1 - sig)))).astype(BF16)
                    return 0

                lax.fori_loop(0, tokens // rows, part, 0)

            at(tL, 2 * NT, back_1)

            def g_pass(u):
                arrived(g_first(u))
                start(g_next(u))

            def g_last(u):
                arrived(g_next(u)[:2])
                start(g_far(u))

            at(tF - 2, 2 * NT, g_pass)
            at(tF - 1, 2 * NT, g_last)

            def back_2(u):
                l, q = 1 - lax.div(u, NT), lax.rem(u, KEEP)

                def part(m, _):
                    r = ds(m * dl, dl)
                    dw[q, r, :] = nn(aT[l, r, :], dgu[...]).astype(BF16)
                    return 0

                lax.fori_loop(0, n, part, 0)

            at(tL, 2 * NT, back_2)

            def add_g(u):
                s, q = lax.rem(u, RING), lax.rem(u, KEEP)
                o = lax.rem(s, KEEP)
                arrived(rg_first(u)[:2])
                og[o, 0] = (wide(l1l[s]) + wide(dw[q, ds(right * dl, half), :])).astype(BF16)
                og[o, 1] = (wide(l1r[s]) + wide(dw[q, ds(left * dl + half, half), :])).astype(BF16)
                start(rg_next(u))

            def add_d(v):
                s = lax.rem(v, RING)
                o = lax.rem(s, KEEP)
                arrived(rd_first(v)[:2])
                done(own_loads(v)[:2])
                od[o, 0] = (wide(k1l[s]) + wide(own[s, pl.ds(0, piece), :])).astype(BF16)
                od[o, 1] = (wide(k1r[s]) + wide(own[s, pl.ds(piece, piece), :])).astype(BF16)
                start(rd_next(v))

            at(tL + 2, 2 * NT, add_g)
            at(tB + 3, 2 * NT, add_d)

            def back_3(u):
                at_, s = dwd_out(u), lax.rem(u, 2)
                dwd[s] = tn(prod[...], y[...]).astype(BF16)
                start(at_)

            at(tL, 2 * NT, back_3)
            at(tL + 1, 2 * NT, lambda u: done(dwd_out(u)))

            def back_4(u):
                s = lax.rem(u, 2)

                def part(m, _):
                    r = ds(m * rows, rows, rows)
                    acc[r, :] += nt(dgu[r, :], wgu_v[s])
                    return 0

                lax.fori_loop(0, tokens // rows, part, 0)

            at(tL, NT, back_4)

            at(tF - 1, 2 * NT, lambda u: arrived(g_next(u)[2:] + g_far(u)))

            k = t + 1 - tF

            @pl.when((k >= 0) & (k < 3 * NT))
            def _():
                start(loads(lax.rem(lax.div(k, NT), 2), lax.rem(k, NT)))

            def total_g(u):
                s, q, f = lax.rem(u, RING), lax.rem(u, KEEP), lax.rem(u, 2)
                arrived(rg_first(u)[2:] + rg_next(u))
                lo = wide(dw[q, ds(me * dl, half), :]) + wide(l3l[s]) + wide(l2r[s])
                hi = wide(dw[q, ds(me * dl + half, half), :]) + wide(l3r[s]) + wide(l2l[s])
                lo, hi = lo.astype(BF16), hi.astype(BF16)
                fg[f, pl.ds(0, half), :] = lo
                fg[f, pl.ds(half, half), :] = hi
                lo, hi = wide(lo), wide(hi)
                sg[...] += jnp.sum((lo * lo + hi * hi).reshape(half // 8, 8, 2 * TILE), 0)
                start(g_out(u))
                sent(rg_first(u) + rg_next(u))

            def total_d(v):
                s, f = lax.rem(v, RING), lax.rem(v, 2)
                arrived(rd_first(v)[2:] + rd_next(v))
                done(own_loads(v)[2:])
                lo = wide(own[s, pl.ds(2 * piece, piece), :]) + wide(k3l[s]) + wide(k2r[s])
                hi = wide(own[s, pl.ds(3 * piece, piece), :]) + wide(k3r[s]) + wide(k2l[s])
                lo, hi = lo.astype(BF16), hi.astype(BF16)
                fd[f, pl.ds(0, piece), :] = lo
                fd[f, pl.ds(piece, piece), :] = hi
                lo, hi = wide(lo), wide(hi)
                sd[...] += jnp.sum((lo * lo + hi * hi).reshape(piece // 8, 8, d), 0)
                start(d_out(v))
                sent(rd_first(v) + rd_next(v))

            at(tL + 4, 2 * NT, lambda u: done(g_out(u)))
            at(tL + 3, 2 * NT, total_g)
            at(tB + 6, 2 * NT, lambda v: done(d_out(v)))
            at(tB + 5, 2 * NT, total_d)
            return 0

        lax.fori_loop(0, end + 1, loop, 0)

        parts = [sg[:, k * 128 : (k + 1) * 128] for k in range(2 * TILE // 128)] + [sd[:, k * 128 : (k + 1) * 128] for k in range(d // 128)]
        st[3] = sum(parts[1:], parts[0])
        sends = [remote(st.at[3], st.at[k], st_s.at[k], st_r.at[k], to) for k, to in enumerate((R, L, O))]
        start(sends)
        done(sends)
        st[4] = st[0] + st[1] + st[2] + st[3]
        last = [local(st.at[4], stat, lin.at[0])]
        start(last)
        done(last)

    any_ = pl.BlockSpec(memory_space=pl.ANY)
    shapes = [
        ((layers, dl, ff), BF16), ((layers, dl, ff), BF16), ((layers, fl, d), BF16), ((8, 128), F32),
        ((layers, NT, d, 2 * TILE), BF16), ((layers, ff, d), BF16), ((layers, ff, d), BF16),
    ]
    V, S = pltpu.VMEM, pltpu.SemaphoreType.DMA
    scratch = [
        V((layers, tokens, d), BF16), V((layers, d, tokens), BF16), V((tokens, d), BF16), V((d, tokens), BF16), V((tokens, d), BF16),
        V((tokens, d), F32), V((tokens, TILE), BF16), V((tokens, 2 * TILE), BF16),
        V((2, d, 2 * TILE), BF16), V((2, TILE, d), BF16), V((KEEP, d, 2 * TILE), BF16), V((2, TILE, d), BF16),
        V((2, dl, 2 * TILE), BF16), V((2, 2 * piece, d), BF16), V((KEEP, 2, half, 2 * TILE), BF16), V((KEEP, 2, piece, d), BF16),
        V((RING, 4 * piece, d), BF16),
    ]
    scratch += [V((RING, half, 2 * TILE), BF16)] * 6 + [V((RING, piece, d), BF16)] * 6
    scratch += [V((8, 2 * TILE), F32), V((8, d), F32), V((5, 8, 128), F32)]
    scratch += [S((7, RING)), S((7, RING)), S((9, RING)), S((9, RING)), S((6, RING)), S((6, RING)), S((6, RING)), S((6, RING))]
    scratch += [S((6, 2)), S((3, RING)), S((3, 2)), S((2,)), S((4,)), S((3,)), S((3,))]
    return pl.pallas_call(
        body,
        out_shape=[jax.ShapeDtypeStruct(*s) for s in shapes],
        in_specs=[any_] * 5,
        out_specs=[any_] * 7,
        scratch_shapes=scratch,
        compiler_params=pltpu.CompilerParams(collective_id=0, has_side_effects=True, vmem_limit_bytes=67043328),
        name="exchange",
    )


def adamw(w, m, v, g):
    m = 0.9 * m + 0.1 * g
    v = 0.95 * v + 0.05 * g * g
    step = m * lax.rsqrt(v + 1e-8) + 0.1 * w
    return (w - 0.02 * step).astype(BF16), m, v


def solution(mesh):
    n = mesh.shape["dp"]

    def step(x, dy, *arrays):
        weights, m, v = (arrays[i : i + 3] for i in (0, 3, 6))
        layers, ff, d = weights[2].shape[0], weights[2].shape[1] * n, weights[2].shape[2]
        *gradients, stat = exchange(n, x.shape[1], d, ff, layers)(x[0], dy[0], *weights)[:4]
        count = n * sum(g.size for g in gradients)
        factor = jnp.minimum(1.0, 0.5 * lax.rsqrt(jnp.sum(stat) / count + 1e-30))
        new = [adamw(w.astype(F32), m, v, g.astype(F32) * factor) for w, m, v, g in zip(weights, m, v, gradients, strict=True)]
        return tuple(one[which] for which in range(3) for one in new)

    states, cut = P(("rep", "dp"), None, None), P(None, "dp", None)
    return jax.shard_map(
        step,
        mesh=mesh,
        in_specs=(states, states) + (cut,) * 9,
        out_specs=(P("rep", "dp", None),) * 9,
        check_vma=False,
    )
```

```python
import jax
import jax.numpy as jnp
from jax import lax
from jax.experimental import pallas as pl
from jax.experimental.pallas import tpu as pltpu
from jax.sharding import PartitionSpec as P

F32, BF16 = jnp.float32, jnp.bfloat16
TILE = 256
RING = 8
TURNS = 12
KEEP = 5
HELD = 4


def nn(a, b):
    return lax.dot_general(a, b, (((1,), (0,)), ((), ())), preferred_element_type=F32)


def nt(a, b):
    return lax.dot_general(a, b, (((1,), (1,)), ((), ())), preferred_element_type=F32)


def exchange(n, tokens, d, ff, layers):
    assert n == 4 and layers == 2
    dl, fl, nt_ = d // n, ff // n, ff // TILE
    half, piece = dl // 2, fl // nt_ // 2
    lent = (half * 3 // 7, half // 2)
    lent_d = (0, piece // 2)
    rows, span = min(512, tokens), min(1024, tokens)
    late = 5
    NT = nt_
    m4 = NT - 3
    assert m4 % 4 == 0 and ff == n * NT * 64

    def tile(j):
        return jnp.where(j < m4, (m4 // 4 + 1) * lax.rem(j, 4) + lax.div(j, 4), (m4 // 4 + 1) * (j - m4) + m4 // 4)

    def unit(block, v):
        return jnp.where(v < m4, block + v, jnp.where(v - m4 < block, v - m4, v))

    def body(
        x, dy, wg, wu, wd,
        gg, gu, gd, stat, WGU, WD, DWD,
        a, aT, y, yT, h, acc, prod, dgu, wgu_v, wd_v, dw, dwd, fg, fd, og, od, own,
        l1l, l1r, l2l, l2r, l3l, l3r, k1l, k1r, k2l, k2r, k3l, k3r, sg, sd, st,
        ad_1, ad_n, ad_a, ad_b, ag_1, ag_n, ag_a, ag_b, rg_s, rg_a, rg_b, rd_s, rd_a, rd_b, ld, lown, lout, lst, lin, st_s, st_r,
    ):
        me, rep = lax.axis_index("dp"), lax.axis_index("rep")
        right, left, far = (lax.rem(me + k, n) for k in (1, n - 1, 2))
        core = lax.rem(rep, 2)
        chip = lax.rem(lax.div(rep, 2), 2)
        R, L, O, C, Y = {"dp": right}, {"dp": left}, {"dp": far}, {"rep": rep + 1 - 2 * core}, {"rep": rep + 2 - 4 * chip}

        def remote(src, dst, ss, rs, to):
            return lambda: pltpu.make_async_remote_copy(
                src_ref=src, dst_ref=dst, send_sem=ss, recv_sem=rs, device_id=to, device_id_type=pl.DeviceIdType.MESH
            )

        def local(src, dst, sem):
            return lambda: pltpu.make_async_copy(src, dst, sem)

        def ds(at, size, by=16):
            return pl.ds(pl.multiple_of(at, by), size)

        barrier = pltpu.get_barrier_semaphore()
        for to in (R, L, O, C, Y):
            pl.semaphore_signal(barrier, inc=1, device_id=to, device_id_type=pl.DeviceIdType.MESH)
        pl.semaphore_wait(barrier, 5)

        def take_g(rows_, sem):
            pltpu.make_async_copy(WGU.at[0, 0, pl.ds(0, rows_)], WGU.at[0, 0, pl.ds(0, rows_)], sem).wait()

        def take_d(rows_, sem):
            pltpu.make_async_copy(WD.at[0, pl.ds(0, rows_)], WD.at[0, pl.ds(0, rows_)], sem).wait()

        class Way:
            def __init__(self, take, first, pass_on, share, whole, got, sent_a, sent_b, sizes):
                lo, hi = pass_on
                self.take, self.got, self.sent_a, self.sent_b, self.sizes = take, got, sent_a, sent_b, sizes
                self.first = [remote(src, dst, sent_a, got[0], to) for src, dst, to in first]
                self.second = [remote(lo, lo, sent_b, got[1], R), remote(hi, hi, sent_b, got[1], L)]
                self.across = [remote(share(b), share(b), sent_b, got[2], Y) for b in (left, right, far)] if sizes[2] else []
                self.inside = [remote(whole(b), whole(b), sent_b, got[3], C) for b in (left, right, far)]

            def go(self, step):
                if step and self.sizes[step - 1]:
                    self.take(self.sizes[step - 1], self.got[step - 1])
                start(((), self.second + self.across[:2], self.across[2:], self.inside, ())[step] if step else self.first)

            def sent_first(self):
                self.take(self.sizes[0], self.sent_a)

            def sent_rest(self):
                self.take(sum(self.sizes[1:]), self.sent_b)

        def d_in(l, j):
            s, few = lax.rem(l * (NT + 1) + j, TURNS), lent_d[l]
            most = piece - few

            def rows_of(block, at, size):
                return ds(block * fl + (2 * unit(block, j) + core) * piece + at, size, 8)

            mine = wd.at[l, ds((2 * unit(me, j) + core) * piece + chip * few, most)]
            to = WD.at[l, rows_of(me, chip * few, most)]
            lo = WD.at[l, rows_of(left, chip * few, most // 2)]
            hi = WD.at[l, rows_of(right, chip * few + most // 2, most // 2)]
            share = lambda b: WD.at[l, rows_of(b, chip * most, few)]
            whole = lambda b: WD.at[l, rows_of(b, 0, piece)]
            got = [ad_1.at[j]] + [ad_n.at[i, s] for i in range(3)]
            sizes = (2 * most, most, 3 * few, 3 * piece)
            return Way(take_d, [(mine, to, R), (mine, to, L)], (lo, hi), share, whole, got, ad_a.at[l, lax.rem(j, TURNS)], ad_b.at[s], sizes)

        def g_in(l, j):
            s, few = lax.rem(l * NT + j, TURNS), lent[l]
            most = half - few

            def rows_of(block, at, size):
                return ds(block * dl + core * half + at, size, 8)

            first = []
            for k, w in enumerate((wg, wu)):
                src = w.at[l, ds(core * half + chip * few, most, 8), ds(tile(j) * TILE, TILE, TILE)]
                dst = WGU.at[l, j, rows_of(me, chip * few, most), pl.ds(k * TILE, TILE)]
                first += [(src, dst, R), (src, dst, L)]
            lo = WGU.at[l, j, rows_of(left, chip * few, most), pl.ds(0, TILE)]
            hi = WGU.at[l, j, rows_of(right, chip * few, most), pl.ds(TILE, TILE)]
            share = lambda b: WGU.at[l, j, rows_of(b, chip * most, few)]
            whole = lambda b: WGU.at[l, j, rows_of(b, 0, half)]
            got = [ag_1.at[j]] + [ag_n.at[i, s] for i in range(3)]
            sizes = (2 * most, most, 3 * few, 3 * half)
            return Way(take_g, first, (lo, hi), share, whole, got, ag_a.at[l, lax.rem(j, TURNS)], ag_b.at[s], sizes)

        def loads(l, j, k):
            s = lax.rem(k, 2)
            out = [
                local(wg.at[l, :, ds(tile(j) * TILE, TILE, TILE)], wgu_v.at[s, ds(me * dl, dl), pl.ds(0, TILE)], ld.at[s]),
                local(wu.at[l, :, ds(tile(j) * TILE, TILE, TILE)], wgu_v.at[s, ds(me * dl, dl), pl.ds(TILE, TILE)], ld.at[s]),
                local(WD.at[l, ds(tile(j) * TILE, TILE)], wd_v.at[s], ld.at[s]),
            ]
            for block in (right, left, far):
                at = ds(block * dl, dl)
                out.append(local(WGU.at[l, j, at], wgu_v.at[s, at], ld.at[s]))
            return out

        def loaded(k):
            take_d(3 * TILE, ld.at[lax.rem(k, 2)])

        def sum_first(src, slot, land, ss, ra, rb):
            return [
                remote(src(far, 0), land[0].at[slot], ss.at[slot], ra.at[slot], R),
                remote(src(far, 1), land[1].at[slot], ss.at[slot], ra.at[slot], L),
                remote(src(right, 1), land[2].at[slot], ss.at[slot], rb.at[slot], R),
                remote(src(left, 0), land[3].at[slot], ss.at[slot], rb.at[slot], L),
            ]

        def sum_next(out, slot, land, ss, rb):
            return [
                remote(out.at[lax.rem(slot, HELD), 0], land[4].at[slot], ss.at[slot], rb.at[slot], R),
                remote(out.at[lax.rem(slot, HELD), 1], land[5].at[slot], ss.at[slot], rb.at[slot], L),
            ]

        land_g, land_d = (l1l, l1r, l2l, l2r, l3l, l3r), (k1l, k1r, k2l, k2r, k3l, k3r)

        def rg_first(u):
            q = lax.rem(u, KEEP)
            return sum_first(lambda b, k: dw.at[q, ds(b * dl + k * half, half)], lax.rem(u, RING), land_g, rg_s, rg_a, rg_b)

        def rg_next(u):
            return sum_next(og, lax.rem(u, RING), land_g, rg_s, rg_b)

        def rd_first(v):
            l, j = 1 - lax.div(v, NT), lax.rem(v, NT)
            at = lambda b, k: DWD.at[l, ds(b * fl + (2 * unit(b, j) + k) * piece, piece)]
            return sum_first(at, lax.rem(v, RING), land_d, rd_s, rd_a, rd_b)

        def rd_next(v):
            return sum_next(od, lax.rem(v, RING), land_d, rd_s, rd_b)

        def own_loads(v):
            l, j, s = 1 - lax.div(v, NT), lax.rem(v, NT), lax.rem(v, RING)
            at = lambda b, k, m: DWD.at[l, ds(b * fl + (2 * unit(b, j) + k) * piece, m * piece)]
            return [
                local(at(right, 0, 1), own.at[s, pl.ds(0, piece)], lown.at[0, s]),
                local(at(left, 1, 1), own.at[s, pl.ds(piece, piece)], lown.at[0, s]),
                local(at(me, 0, 2), own.at[s, pl.ds(2 * piece, 2 * piece)], lown.at[1, s]),
            ]

        def g_out(u):
            l, j, s = 1 - lax.div(u, NT), lax.rem(u, NT), lax.rem(u, 2)
            to = ds(tile(j) * TILE, TILE, TILE)
            return [
                local(fg.at[s, :, pl.ds(0, TILE)], gg.at[l, :, to], lout.at[0, s]),
                local(fg.at[s, :, pl.ds(TILE, TILE)], gu.at[l, :, to], lout.at[0, s]),
            ]

        def d_out(v):
            l, j, s = 1 - lax.div(v, NT), lax.rem(v, NT), lax.rem(v, 2)
            return [local(fd.at[s], gd.at[l, ds(unit(me, j) * 2 * piece, 2 * piece)], lout.at[1, s])]

        def dwd_out(u):
            l, j, s = 1 - lax.div(u, NT), lax.rem(u, NT), lax.rem(u, 2)
            return [local(dwd.at[s], DWD.at[l, ds(tile(j) * TILE, TILE)], lst.at[s])]

        def start(copies):
            for c in copies:
                c().start()

        def done(copies):
            for c in copies:
                c().wait()

        def wide(ref):
            return ref.astype(F32)

        tF = 7
        tL, tB, tE = tF + NT, tF + 2 * NT, tF + 3 * NT
        end = tE + 9
        blk = min(256, tokens)
        nblk = tokens // blk

        aside = a.at[1, pl.ds(0, fl)]
        own_w = [[local(wd.at[l], aside, lin.at[0])] for l in range(layers)]
        put_w = [[local(aside, WD.at[l, ds(me * fl, fl)], lin.at[0])] for l in range(layers)]
        own_x = [local(x, h, lin.at[1]), local(dy, y, lin.at[2])]

        def norm_into(l, r):
            hw = wide(h[r, :])
            scale = lax.rsqrt(jnp.mean(hw * hw, -1, keepdims=True) + 1e-6)
            n_ = (hw * scale).astype(BF16)
            a[l, r, :] = n_
            aT[l, :, r] = n_.T

        def loop(t, _):
            def at(t0, count, f):
                k = t - t0

                @pl.when((k >= 0) & (k < count))
                def _():
                    f(k)

            def ramp(ahead, more, f, late=0):
                lo, hi = (jnp.clip(s - tF + ahead + jnp.clip(s - tF - late, 0, more), 0, NT) for s in (t, t + 1))

                @pl.when(hi > lo)
                def _():
                    def one(j, _):
                        f(j)
                        return 0

                    lax.fori_loop(lo, hi, one, 0)

            def at4(t0, f):
                k = t - t0

                @pl.when((k >= 0) & (k < NT) & (lax.rem(k, 4) == 0))
                def _():
                    def one(v, _):
                        f(v)
                        return 0

                    lax.fori_loop(k, jnp.minimum(k + 4, NT), one, 0)

            at(tF - 4, NT, lambda j: g_in(0, j).sent_first())
            at4(tF - 4, lambda j: d_in(0, j).sent_first())
            for l in range(layers):
                at(tF + l * NT + 1, NT, lambda j: g_in(l, j).sent_rest())
                at4(tF + l * NT, lambda j: d_in(l, j).sent_rest())
            at4(tF - 7, lambda j: d_in(0, j).go(0))
            ramp(6, 4, lambda j: g_in(0, j).go(0))

            def early(j):
                g_in(1, j).go(0)
                d_in(1, j).go(0)

            def early_sent(j):
                g_in(1, j).sent_first()
                d_in(1, j).sent_first()

            at(tF + 8, NT - late, early_sent)
            at(tL + 4, late, lambda j: early_sent(NT - late + j))
            at(tF + 5, NT - late, early)

            @pl.when(t == tL)
            def _():
                def one(j, _):
                    early(j)
                    return 0

                lax.fori_loop(NT - late, NT, one, 0)

            at(tL + 1, 2 * NT, lambda u: start(rg_first(u)))
            at(tL + 5, 2 * NT, lambda v: start(rd_first(v) + own_loads(v)))

            @pl.when(t == 0)
            def _():
                start(own_x + own_w[0])
                acc[...] = jnp.zeros_like(acc)
                sg[...] = jnp.zeros_like(sg)
                sd[...] = jnp.zeros_like(sd)
                done(own_x)

                def begin(m, _):
                    r = ds(m * blk, blk, blk)
                    norm_into(0, r)
                    yT[:, r] = y[r, :].T
                    return 0

                lax.fori_loop(0, nblk, begin, 0)
                done(own_w[0])
                start(put_w[0])

            @pl.when(t == 1)
            def _():
                done(put_w[0])
                start(own_w[1])

            @pl.when(t == 2)
            def _():
                done(own_w[1])
                start(put_w[1])

            @pl.when(t == 3)
            def _():
                done(put_w[1])

            for l in range(layers):
                at(tF + l * NT - 1, NT, lambda j: g_in(l, j).go(4))
                at4(tF + l * NT - 1, lambda j: d_in(l, j).go(4))

            k = t + 1 - tF

            @pl.when((k >= 0) & (k < 3 * NT))
            def _():
                start(loads(lax.rem(lax.div(k, NT), 2), lax.rem(k, NT), k))

            @pl.when(t == tL)
            def _():
                def piece_(m, _):
                    r = ds(m * blk, blk, blk)
                    h[r, :] = (wide(h[r, :]) + wide(acc[r, :].astype(BF16))).astype(BF16)
                    acc[r, :] = jnp.zeros((blk, d), F32)
                    norm_into(1, r)
                    return 0

                lax.fori_loop(0, nblk, piece_, 0)

            @pl.when(t == tB)
            def _():
                def piece_(m, _):
                    r = ds(m * blk, blk, blk)
                    hw, da = wide(h[r, :]), wide(acc[r, :].astype(BF16))
                    scale = lax.rsqrt(jnp.mean(hw * hw, -1, keepdims=True) + 1e-6)
                    by_scale = jnp.sum(da * hw, -1, keepdims=True)
                    by_h = (da * scale - hw * (by_scale * scale * scale * scale * (1.0 / d))).astype(BF16)
                    by = (wide(y[r, :]) + wide(by_h)).astype(BF16)
                    y[r, :] = by
                    yT[:, r] = by.T
                    return 0

                lax.fori_loop(0, nblk, piece_, 0)

            def forward(j):
                s = lax.rem(j, 2)
                loaded(j)

                for m in range(tokens // span):
                    r = pl.ds(m * span, span)
                    both = nn(a[0, r, :], wgu_v[s])
                    gate, up = both[:, :TILE], both[:, TILE:]
                    p = (gate * (1 / (1 + jnp.exp(-gate))) * up).astype(BF16)
                    acc[r, :] += nn(p, wd_v[s])

            at(tF, NT, forward)

            def back_1(u):
                l, s = 1 - lax.div(u, NT), lax.rem(u + NT, 2)
                loaded(u + NT)

                for m in range(tokens // rows):
                    r = pl.ds(m * rows, rows)
                    both = nn(a[l, r, :], wgu_v[s])
                    gate, up = both[:, :TILE], both[:, TILE:]
                    by = wide(nt(y[r, :], wd_v[s]).astype(BF16))
                    sig = 1 / (1 + jnp.exp(-gate))
                    act = gate * sig
                    prod[r, :] = (act * up).astype(BF16)
                    dgu[r, TILE:] = (by * act).astype(BF16)
                    dgu[r, :TILE] = (by * up * (sig * (1 + gate * (1 - sig)))).astype(BF16)

            at(tL, 2 * NT, back_1)

            for k, ahead, more in ((3, 3, 1), (2, 4, 2), (1, 5, 3)):
                ramp(ahead, more, lambda j: g_in(0, j).go(k), k)
                if k == 2:
                    at4(tF - 3, lambda j: (d_in(0, j).go(2), d_in(0, j).go(3)))
                if k == 1:
                    at4(tF - 5, lambda j: d_in(0, j).go(1))
                at(tL - ahead - more, NT, lambda j: g_in(1, j).go(k))
                at4(tL - ahead - more, lambda j: d_in(1, j).go(k))

            def back_2(u):
                l, q = 1 - lax.div(u, NT), lax.rem(u, KEEP)

                dw[q] = nn(aT[l], dgu[...]).astype(BF16)

            at(tL, 2 * NT, back_2)

            def add_g(u):
                s, q = lax.rem(u, RING), lax.rem(u, KEEP)
                o = lax.rem(s, HELD)
                take_g(2 * half, rg_a.at[s])
                og[o, 0] = (wide(l1l[s]) + wide(dw[q, ds(right * dl, half), :])).astype(BF16)
                og[o, 1] = (wide(l1r[s]) + wide(dw[q, ds(left * dl + half, half), :])).astype(BF16)
                start(rg_next(u))

            def add_d(v):
                s = lax.rem(v, RING)
                o = lax.rem(s, HELD)
                take_d(2 * piece, rd_a.at[s])
                take_d(2 * piece, lown.at[0, s])
                od[o, 0] = (wide(k1l[s]) + wide(own[s, pl.ds(0, piece), :])).astype(BF16)
                od[o, 1] = (wide(k1r[s]) + wide(own[s, pl.ds(piece, piece), :])).astype(BF16)
                start(rd_next(v))

            at(tL + 2, 2 * NT, add_g)
            at(tL + 7, 2 * NT, add_d)

            def back_3(u):
                at_, s = dwd_out(u), lax.rem(u, 2)
                dwd[s] = nn(yT[...], prod[...]).astype(BF16).T
                start(at_)

            at(tL, 2 * NT, back_3)
            at(tL + 1, 2 * NT, lambda u: done(dwd_out(u)))

            def back_4(u):
                s = lax.rem(u + NT, 2)

                def part(m, _):
                    r = ds(m * span, span, span)
                    acc[r, :] += nt(dgu[r, :], wgu_v[s])
                    return 0

                lax.fori_loop(0, tokens // span, part, 0)

            at(tL, NT, back_4)

            def total_g(u):
                s, q, f = lax.rem(u, RING), lax.rem(u, KEEP), lax.rem(u, 2)
                take_g(4 * half, rg_b.at[s])
                lo = wide(dw[q, ds(me * dl, half), :]) + wide(l3l[s]) + wide(l2r[s])
                hi = wide(dw[q, ds(me * dl + half, half), :]) + wide(l3r[s]) + wide(l2l[s])
                lo, hi = lo.astype(BF16), hi.astype(BF16)
                fg[f, pl.ds(0, half), :] = lo
                fg[f, pl.ds(half, half), :] = hi
                lo, hi = wide(lo), wide(hi)
                sg[...] += jnp.sum((lo * lo + hi * hi).reshape(half // 8, 8, 2 * TILE), 0)
                start(g_out(u))
                take_g(6 * half, rg_s.at[s])

            def total_d(v):
                s, f = lax.rem(v, RING), lax.rem(v, 2)
                take_d(4 * piece, rd_b.at[s])
                take_d(2 * piece, lown.at[1, s])
                lo = wide(own[s, pl.ds(2 * piece, piece), :]) + wide(k3l[s]) + wide(k2r[s])
                hi = wide(own[s, pl.ds(3 * piece, piece), :]) + wide(k3r[s]) + wide(k2l[s])
                lo, hi = lo.astype(BF16), hi.astype(BF16)
                fd[f, pl.ds(0, piece), :] = lo
                fd[f, pl.ds(piece, piece), :] = hi
                lo, hi = wide(lo), wide(hi)
                sd[...] += jnp.sum((lo * lo + hi * hi).reshape(piece // 8, 8, d), 0)
                start(d_out(v))
                take_d(6 * piece, rd_s.at[s])

            at(tL + 5, 2 * NT, lambda u: take_g(dl, lout.at[0, lax.rem(u, 2)]))
            at(tL + 4, 2 * NT, total_g)
            at(tL + 10, 2 * NT, lambda v: done(d_out(v)))
            at(tL + 9, 2 * NT, total_d)
            return 0

        lax.fori_loop(0, end + 1, loop, 0)

        parts = [sg[:, k * 128 : (k + 1) * 128] for k in range(2 * TILE // 128)] + [sd[:, k * 128 : (k + 1) * 128] for k in range(d // 128)]
        st[3] = sum(parts[1:], parts[0])
        sends = [remote(st.at[3], st.at[k], st_s.at[k], st_r.at[k], to) for k, to in enumerate((R, L, O))]
        start(sends)
        done(sends)
        st[4] = st[0] + st[1] + st[2] + st[3]
        last = [local(st.at[4], stat, lin.at[0])]
        start(last)
        done(last)

    any_ = pl.BlockSpec(memory_space=pl.ANY)
    shapes = [
        ((layers, dl, ff), BF16), ((layers, dl, ff), BF16), ((layers, fl, d), BF16), ((8, 128), F32),
        ((layers, NT, d, 2 * TILE), BF16), ((layers, ff, d), BF16), ((layers, ff, d), BF16),
    ]
    V, S = pltpu.VMEM, pltpu.SemaphoreType.DMA
    scratch = [
        V((layers, tokens, d), BF16), V((layers, d, tokens), BF16), V((tokens, d), BF16), V((d, tokens), BF16), V((tokens, d), BF16),
        V((tokens, d), F32), V((tokens, TILE), BF16), V((tokens, 2 * TILE), BF16),
        V((2, d, 2 * TILE), BF16), V((2, TILE, d), BF16), V((KEEP, d, 2 * TILE), BF16), V((2, TILE, d), BF16),
        V((2, dl, 2 * TILE), BF16), V((2, 2 * piece, d), BF16), V((HELD, 2, half, 2 * TILE), BF16), V((HELD, 2, piece, d), BF16),
        V((RING, 4 * piece, d), BF16),
    ]
    scratch += [V((RING, half, 2 * TILE), BF16)] * 6 + [V((RING, piece, d), BF16)] * 6
    scratch += [V((8, 2 * TILE), F32), V((8, d), F32), V((5, 8, 128), F32)]
    way = [S((NT,)), S((3, TURNS)), S((layers, TURNS)), S((TURNS,))]
    scratch += way + way + [S((RING,))] * 6
    scratch += [S((2,)), S((2, RING)), S((2, 2)), S((2,)), S((3,)), S((3,)), S((3,))]
    return pl.pallas_call(
        body,
        out_shape=[jax.ShapeDtypeStruct(*s) for s in shapes],
        in_specs=[any_] * 5,
        out_specs=[any_] * 7,
        scratch_shapes=scratch,
        compiler_params=pltpu.CompilerParams(collective_id=0, has_side_effects=True, vmem_limit_bytes=67043328),
        name="exchange",
    )


def adamw(n, layers, dl, ff, fl, d):
    count = n * layers * (2 * dl * ff + fl * d)
    steps = 8

    def body(stat, *refs):
        ins, outs = refs[:12], refs[12:]
        factor = jnp.minimum(1.0, 0.5 * lax.rsqrt(jnp.sum(stat[...]) / count + 1e-30))
        for i in range(3):
            g, w, m, v = (ins[4 * i + k] for k in range(4))
            by = g[...].astype(F32) * factor
            first = 0.9 * m[...] + 0.1 * by
            second = 0.95 * v[...] + 0.05 * by * by
            old = w[...].astype(F32)
            outs[i][...] = (old - 0.02 * (first * lax.rsqrt(second + 1e-8) + 0.1 * old)).astype(BF16)
            outs[3 + i][...] = first
            outs[6 + i][...] = second

    sizes = [(layers * dl, ff), (layers * dl, ff), (layers * fl, d)]
    kinds = [pl.BlockSpec((rows // steps, columns), lambda i: (i, 0)) for rows, columns in sizes]
    call = pl.pallas_call(
        body,
        grid=(steps,),
        in_specs=[pl.BlockSpec((8, 128), lambda i: (0, 0))] + [k for k in kinds for _ in range(4)],
        out_specs=kinds * 3,
        out_shape=[jax.ShapeDtypeStruct(s, t) for t in (BF16, F32, F32) for s in sizes],
        compiler_params=pltpu.CompilerParams(vmem_limit_bytes=67043328),
        name="adamw",
    )

    def run(stat, gradients, weights, m, v):
        flat = [one.reshape(-1, one.shape[-1]) for four in zip(gradients, weights, m, v, strict=True) for one in four]
        shapes = [w.shape for w in weights] * 3
        return tuple(out.reshape(s) for out, s in zip(call(stat, *flat), shapes, strict=True))

    return run


def solution(mesh):
    n = mesh.shape["dp"]

    def step(x, dy, *arrays):
        weights, m, v = (arrays[i : i + 3] for i in (0, 3, 6))
        layers, ff, d = weights[2].shape[0], weights[2].shape[1] * n, weights[2].shape[2]
        *gradients, stat = exchange(n, x.shape[1], d, ff, layers)(x[0], dy[0], *weights)[:4]
        return adamw(n, layers, d // n, ff, ff // n, d)(stat, gradients, weights, m, v)

    states, cut = P(("rep", "dp"), None, None), P(None, "dp", None)
    return jax.shard_map(
        step,
        mesh=mesh,
        in_specs=(states, states) + (cut,) * 9,
        out_specs=(P("rep", "dp", None),) * 9,
        check_vma=False,
    )
```

```python
import jax
import jax.numpy as jnp
from jax import lax
from jax.experimental import pallas as pl
from jax.experimental.pallas import tpu as pltpu
from jax.sharding import PartitionSpec as P

F32, BF16 = jnp.float32, jnp.bfloat16
TILE = 256
RING = 8
TURNS = 12
KEEP = 4
HELD = 4


def nn(a, b):
    return lax.dot_general(a, b, (((1,), (0,)), ((), ())), preferred_element_type=F32)


def nt(a, b):
    return lax.dot_general(a, b, (((1,), (1,)), ((), ())), preferred_element_type=F32)


def exchange(n, tokens, d, ff, layers):
    assert n == 4 and layers == 2
    dl, fl, nt_ = d // n, ff // n, ff // TILE
    half, piece = dl // 2, fl // nt_ // 2
    lent = (half * 2 // 7, half // 2)
    lent_d = piece // 2
    rows, span = min(512, tokens), min(1024, tokens)
    begin = 6
    late = 5
    NT = nt_
    m4 = NT - 3
    assert m4 % 4 == 0 and ff == n * NT * 64

    def tile(j):
        return jnp.where(j < m4, (m4 // 4 + 1) * lax.rem(j, 4) + lax.div(j, 4), (m4 // 4 + 1) * (j - m4) + m4 // 4)

    def unit(block, v):
        return jnp.where(v < m4, block + v, jnp.where(v - m4 < block, v - m4, v))

    def body(
        x, dy, wg, wu, wd,
        gg, gu, gd, stat, WGU, WD, DWD,
        a, aT, y, yT, h, acc, prod, dgu, wgu_v, wd_v, dw, dwd, fg, fd, og, od, own,
        l1l, l1r, l2l, l2r, l3l, l3r, k1l, k1r, k2l, k2r, k3l, k3r, sg, sd, st,
        ad_1, ad_n, ad_a, ad_b, ag_1, ag_n, ag_a, ag_b, rg_s, rg_a, rg_b, rd_s, rd_a, rd_b, ld, lown, lout, lst, lin, st_s, st_r,
    ):
        me, rep = lax.axis_index("dp"), lax.axis_index("rep")
        right, left, far = (lax.rem(me + k, n) for k in (1, n - 1, 2))
        core = lax.rem(rep, 2)
        chip = lax.rem(lax.div(rep, 2), 2)
        R, L, O, C, Y = {"dp": right}, {"dp": left}, {"dp": far}, {"rep": rep + 1 - 2 * core}, {"rep": rep + 2 - 4 * chip}

        def remote(src, dst, ss, rs, to):
            return lambda: pltpu.make_async_remote_copy(
                src_ref=src, dst_ref=dst, send_sem=ss, recv_sem=rs, device_id=to, device_id_type=pl.DeviceIdType.MESH
            )

        def local(src, dst, sem):
            return lambda: pltpu.make_async_copy(src, dst, sem)

        def ds(at, size, by=16):
            return pl.ds(pl.multiple_of(at, by), size)

        barrier = pltpu.get_barrier_semaphore()
        for to in (R, L, O, C, Y):
            pl.semaphore_signal(barrier, inc=1, device_id=to, device_id_type=pl.DeviceIdType.MESH)
        pl.semaphore_wait(barrier, 5)

        def take_g(rows_, sem):
            pltpu.make_async_copy(WGU.at[0, 0, pl.ds(0, rows_)], WGU.at[0, 0, pl.ds(0, rows_)], sem).wait()

        def take_d(rows_, sem):
            pltpu.make_async_copy(WD.at[0, pl.ds(0, rows_)], WD.at[0, pl.ds(0, rows_)], sem).wait()

        class Way:
            def __init__(self, take, first, pass_on, share, whole, got, sent_a, sent_b, sizes, soon):
                lo, hi = pass_on
                self.soon = soon
                self.take, self.got, self.sent_a, self.sent_b, self.sizes = take, got, sent_a, sent_b, sizes
                self.first = [remote(src, dst, sent_a, got[0], to) for src, dst, to in first]
                self.second = [remote(lo, lo, sent_b, got[1], R), remote(hi, hi, sent_b, got[1], L)]
                self.across = [remote(share(b), share(b), sent_b, got[2], Y) for b in (left, right, far)] if sizes[2] else []
                self.inside = [remote(whole(b), whole(b), sent_b, got[3], C) for b in (left, right, far)]

            def go(self, step):
                if step and self.sizes[step - 1]:
                    self.take(self.sizes[step - 1], self.got[step - 1])
                k = 2 if self.soon else 0
                start((self.first, self.second + self.across[:k], self.across[k:], self.inside, ())[step])

            def sent_first(self):
                self.take(self.sizes[0], self.sent_a)

            def sent_rest(self):
                self.take(sum(self.sizes[1:]), self.sent_b)

        def d_in(l, j, many, few=lent_d):
            s, few, part = lax.rem(l * (NT + 1) + j, TURNS), many * few, many * piece
            most = part - few

            def rows_of(block, at, size):
                return ds(block * fl + 2 * piece * unit(block, j) + part * core + at, size, 8)

            mine = wd.at[l, ds(2 * piece * unit(me, j) + part * core + chip * few, most)]
            to = WD.at[l, rows_of(me, chip * few, most)]
            lo = WD.at[l, rows_of(left, chip * few, most // 2)]
            hi = WD.at[l, rows_of(right, chip * few + most // 2, most // 2)]
            share = lambda b: WD.at[l, rows_of(b, chip * most, few)]
            whole = lambda b: WD.at[l, rows_of(b, 0, part)]
            got = [ad_1.at[j]] + [ad_n.at[i, s] for i in range(3)]
            sizes = (2 * most, most, 3 * few, 3 * part)
            return Way(take_d, [(mine, to, R), (mine, to, L)], (lo, hi), share, whole, got, ad_a.at[l, lax.rem(j, TURNS)], ad_b.at[s], sizes, l == 0)

        def g_in(l, j):
            s, few = lax.rem(l * NT + j, TURNS), lent[l]
            most = half - few

            def rows_of(block, at, size):
                return ds(block * dl + core * half + at, size, 8)

            first = []
            for k, w in enumerate((wg, wu)):
                src = w.at[l, ds(core * half + chip * few, most, 8), ds(tile(j) * TILE, TILE, TILE)]
                dst = WGU.at[l, j, rows_of(me, chip * few, most), pl.ds(k * TILE, TILE)]
                first += [(src, dst, R), (src, dst, L)]
            lo = WGU.at[l, j, rows_of(left, chip * few, most), pl.ds(0, TILE)]
            hi = WGU.at[l, j, rows_of(right, chip * few, most), pl.ds(TILE, TILE)]
            share = lambda b: WGU.at[l, j, rows_of(b, chip * most, few)]
            whole = lambda b: WGU.at[l, j, rows_of(b, 0, half)]
            got = [ag_1.at[j]] + [ag_n.at[i, s] for i in range(3)]
            sizes = (2 * most, most, 3 * few, 3 * half)
            return Way(take_g, first, (lo, hi), share, whole, got, ag_a.at[l, lax.rem(j, TURNS)], ag_b.at[s], sizes, l == 0)

        def loads(l, j, k):
            s = lax.rem(k, 2)
            out = [
                local(wg.at[l, :, ds(tile(j) * TILE, TILE, TILE)], wgu_v.at[s, ds(me * dl, dl), pl.ds(0, TILE)], ld.at[s]),
                local(wu.at[l, :, ds(tile(j) * TILE, TILE, TILE)], wgu_v.at[s, ds(me * dl, dl), pl.ds(TILE, TILE)], ld.at[s]),
                local(WD.at[l, ds(tile(j) * TILE, TILE)], wd_v.at[s], ld.at[s]),
            ]
            for block in (right, left, far):
                at = ds(block * dl, dl)
                out.append(local(WGU.at[l, j, at], wgu_v.at[s, at], ld.at[s]))
            return out

        def loaded(k):
            take_d(3 * TILE, ld.at[lax.rem(k, 2)])

        def sum_first(src, slot, land, ss, ra, rb):
            return [
                remote(src(far, 0), land[0].at[slot], ss.at[slot], ra.at[slot], R),
                remote(src(far, 1), land[1].at[slot], ss.at[slot], ra.at[slot], L),
                remote(src(right, 1), land[2].at[slot], ss.at[slot], rb.at[slot], R),
                remote(src(left, 0), land[3].at[slot], ss.at[slot], rb.at[slot], L),
            ]

        def sum_next(out, slot, land, ss, rb):
            return [
                remote(out.at[lax.rem(slot, HELD), 0], land[4].at[slot], ss.at[slot], rb.at[slot], R),
                remote(out.at[lax.rem(slot, HELD), 1], land[5].at[slot], ss.at[slot], rb.at[slot], L),
            ]

        land_g, land_d = (l1l, l1r, l2l, l2r, l3l, l3r), (k1l, k1r, k2l, k2r, k3l, k3r)

        def rg_first(u):
            q = lax.rem(u, KEEP)
            return sum_first(lambda b, k: dw.at[q, ds(b * dl + k * half, half)], lax.rem(u, RING), land_g, rg_s, rg_a, rg_b)

        def rg_next(u):
            return sum_next(og, lax.rem(u, RING), land_g, rg_s, rg_b)

        def rd_first(v):
            l, j = 1 - lax.div(v, NT), lax.rem(v, NT)
            at = lambda b, k: DWD.at[l, ds(b * fl + (2 * unit(b, j) + k) * piece, piece)]
            return sum_first(at, lax.rem(v, RING), land_d, rd_s, rd_a, rd_b)

        def rd_next(v):
            return sum_next(od, lax.rem(v, RING), land_d, rd_s, rd_b)

        def own_loads(v):
            l, j, s = 1 - lax.div(v, NT), lax.rem(v, NT), lax.rem(v, RING)
            at = lambda b, k, m: DWD.at[l, ds(b * fl + (2 * unit(b, j) + k) * piece, m * piece)]
            return [
                local(at(right, 0, 1), own.at[s, pl.ds(0, piece)], lown.at[0, s]),
                local(at(left, 1, 1), own.at[s, pl.ds(piece, piece)], lown.at[0, s]),
                local(at(me, 0, 2), own.at[s, pl.ds(2 * piece, 2 * piece)], lown.at[1, s]),
            ]

        def g_out(u):
            l, j, s = 1 - lax.div(u, NT), lax.rem(u, NT), lax.rem(u, 2)
            to = ds(tile(j) * TILE, TILE, TILE)
            return [
                local(fg.at[s, :, pl.ds(0, TILE)], gg.at[l, :, to], lout.at[0, s]),
                local(fg.at[s, :, pl.ds(TILE, TILE)], gu.at[l, :, to], lout.at[0, s]),
            ]

        def d_out(v):
            l, j, s = 1 - lax.div(v, NT), lax.rem(v, NT), lax.rem(v, 2)
            return [local(fd.at[s], gd.at[l, ds(unit(me, j) * 2 * piece, 2 * piece)], lout.at[1, s])]

        def dwd_out(u):
            l, j, s = 1 - lax.div(u, NT), lax.rem(u, NT), lax.rem(u, 2)
            return [local(dwd.at[s], DWD.at[l, ds(tile(j) * TILE, TILE)], lst.at[s])]

        def start(copies):
            for c in copies:
                c().start()

        def done(copies):
            for c in copies:
                c().wait()

        def wide(ref):
            return ref.astype(F32)

        tF = 7
        tL, tB, tE = tF + NT, tF + 2 * NT, tF + 3 * NT
        end = tE + 8
        blk = min(256, tokens)
        nblk = tokens // blk

        aside = a.at[1, pl.ds(0, fl)]
        own_w = [[local(wd.at[l], aside, lin.at[0])] for l in range(layers)]
        put_w = [[local(aside, WD.at[l, ds(me * fl, fl)], lin.at[0])] for l in range(layers)]
        own_x = [local(x, h, lin.at[1]), local(dy, y, lin.at[2])]

        def norm_into(l, r):
            hw = wide(h[r, :])
            scale = lax.rsqrt(jnp.mean(hw * hw, -1, keepdims=True) + 1e-6)
            n_ = (hw * scale).astype(BF16)
            a[l, r, :] = n_
            aT[l, :, r] = n_.T

        def loop(t, lo_, hi_):
            def when(*terms, within=(0, end + 1)):
                if within[0] >= hi_ or within[1] <= lo_:
                    return lambda f: None
                if within[0] <= lo_ and within[1] >= hi_ and not terms:
                    return lambda f: f()
                test = (t >= within[0]) & (t < within[1])
                for term in terms:
                    test = test & term
                return pl.when(test)

            def at(t0, count, f):
                when(*([t >= 0] if f in products else []), within=(t0, t0 + count))(lambda: f(t - t0))

            products = []

            def product(f):
                products.append(f)
                return f

            def once(t0):
                return when(within=(t0, t0 + 1))

            def ramp(ahead, more, f, late=0):
                lo, hi = (
                    jnp.clip(s - tF + ahead + jnp.clip(s - tF - late, 0, more) - jnp.where((s == tF) & (late == 3), 1, 0), 0, NT) for s in (t, t + 1)
                )

                when(hi > lo + 1, within=(tF - ahead, tL))(lambda: f(lo))
                when(hi > lo, within=(tF - ahead, tL))(lambda: f(hi - 1))

            def at4(l, first, then, f, only=None):
                if only != "then":
                    once(first)(lambda: f(d_in(l, 0, 4, 0)))
                if only != "first":
                    k = t - then
                    when(lax.rem(k, 4) == 0, within=(then + 1, then + m4))(lambda: f(d_in(l, k, 4)))

                    @once(then + m4)
                    def _():
                        def one(v, _):
                            f(d_in(l, v, 1))
                            return 0

                        lax.fori_loop(m4, NT, one, 0)

            at(tF - 4, NT, lambda j: g_in(0, j).sent_first())
            at4(0, tF - 4, tF - 4, lambda w: w.sent_first())
            for l in range(layers):
                at(tF + l * NT + 1, NT, lambda j: g_in(l, j).sent_rest())
                at4(l, tF + l * NT, tF + l * NT, lambda w: w.sent_rest())
            at4(0, tF - 7, tF - 8, lambda w: w.go(0))
            ramp(6, 4, lambda j: g_in(0, j).go(0))

            at(tF + begin + 4, NT - late, lambda j: g_in(1, j).sent_first())
            at(tL + 4, late, lambda j: g_in(1, NT - late + j).sent_first())
            at4(1, tF + begin + 4, tF + begin + 4, lambda w: w.sent_first())
            at(tF + begin, NT - late, lambda j: g_in(1, j).go(0))
            at4(1, tF + begin, tF + begin, lambda w: w.go(0))

            @once(tL)
            def _():
                def one(j, _):
                    g_in(1, j).go(0)
                    return 0

                lax.fori_loop(NT - late, NT, one, 0)

            at(tL + 1, 2 * NT, lambda u: done(dwd_out(u)))
            at(tL + 4, 2 * NT, lambda v: start(rd_first(v) + own_loads(v)))

            @once(0)
            def _():
                start(own_x + own_w[0])
                acc[...] = jnp.zeros_like(acc)
                sg[...] = jnp.zeros_like(sg)
                sd[...] = jnp.zeros_like(sd)

            @once(1)
            def _():
                done(own_x)

                def start_on(m, _):
                    r = ds(m * blk, blk, blk)
                    norm_into(0, r)
                    yT[:, r] = y[r, :].T
                    return 0

                lax.fori_loop(0, nblk, start_on, 0)
                done(own_w[0])
                start(put_w[0])

            @once(2)
            def _():
                done(put_w[0])
                start(own_w[1])

            @once(3)
            def _():
                done(own_w[1])
                start(put_w[1])

            @once(4)
            def _():
                done(put_w[1])

            @once(tL)
            def _():
                def piece_(m, _):
                    r = ds(m * blk, blk, blk)
                    h[r, :] = (wide(h[r, :]) + wide(acc[r, :].astype(BF16))).astype(BF16)
                    acc[r, :] = jnp.zeros((blk, d), F32)
                    norm_into(1, r)
                    return 0

                lax.fori_loop(0, nblk, piece_, 0)

            @once(tB)
            def _():
                def piece_(m, _):
                    r = ds(m * blk, blk, blk)
                    hw, da = wide(h[r, :]), wide(acc[r, :].astype(BF16))
                    scale = lax.rsqrt(jnp.mean(hw * hw, -1, keepdims=True) + 1e-6)
                    by_scale = jnp.sum(da * hw, -1, keepdims=True)
                    by_h = (da * scale - hw * (by_scale * scale * scale * scale * (1.0 / d))).astype(BF16)
                    by = (wide(y[r, :]) + wide(by_h)).astype(BF16)
                    y[r, :] = by
                    yT[:, r] = by.T
                    return 0

                lax.fori_loop(0, nblk, piece_, 0)

            for l in range(layers):
                at(tF + l * NT - 1, NT, lambda j: g_in(l, j).go(4))

            for l in range(layers):
                at4(l, tF + l * NT - 1, tF + l * NT - 1, lambda w: w.go(4))

            k = t + 1 - tF

            @when(within=(tF - 1, tE - 1))
            def _():
                start(loads(lax.rem(lax.div(k, NT), 2), lax.rem(k, NT), k))

            @product
            def forward(j):
                s = lax.rem(j, 2)
                loaded(j)

                for m in range(tokens // span):
                    r = pl.ds(m * span, span)
                    both = nn(a[0, r, :], wgu_v[s])
                    gate, up = both[:, :TILE], both[:, TILE:]
                    p = (gate * (1 / (1 + jnp.exp(-gate))) * up).astype(BF16)
                    acc[r, :] += nn(p, wd_v[s])

            at(tF, NT, forward)

            @product
            def back_1(u):
                l, s = 1 - lax.div(u, NT), lax.rem(u + NT, 2)
                loaded(u + NT)

                for m in range(tokens // rows):
                    r = pl.ds(m * rows, rows)
                    both = nn(a[l, r, :], wgu_v[s])
                    gate, up = both[:, :TILE], both[:, TILE:]
                    by = wide(nt(y[r, :], wd_v[s]).astype(BF16))
                    sig = 1 / (1 + jnp.exp(-gate))
                    act = gate * sig
                    prod[r, :] = (act * up).astype(BF16)
                    dgu[r, TILE:] = (by * act).astype(BF16)
                    dgu[r, :TILE] = (by * up * (sig * (1 + gate * (1 - sig)))).astype(BF16)

            at(tL, 2 * NT, back_1)

            for k, ahead, more, ahead_0, ahead_d, ahead_1 in ((3, 3, 1, 3, 3, 2), (2, 4, 2, 3, 4, 6), (1, 5, 3, 5, 6, 8)):
                ramp(ahead, more, lambda j: g_in(0, j).go(k), k)
                at4(0, tF - ahead_0, tF - ahead_d, lambda w: w.go(k), "then" if k == 3 else None)
                if k == 2:
                    at4(0, tF - ahead_0, tF - ahead_d, lambda w: w.go(3), "first")
                at(tL - ahead_1, NT, lambda j: g_in(1, j).go(k))
                at4(1, tL - ahead_1, tL - ahead_1, lambda w: w.go(k))

            @product
            def back_2(u):
                l, q = 1 - lax.div(u, NT), lax.rem(u, KEEP)

                dw[q] = nn(aT[l], dgu[...]).astype(BF16)

            at(tL, 2 * NT, back_2)

            @product
            def add_g(u):
                s, q = lax.rem(u, RING), lax.rem(u, KEEP)
                o = lax.rem(s, HELD)
                take_g(2 * half, rg_a.at[s])
                og[o, 0] = (wide(l1l[s]) + wide(dw[q, ds(right * dl, half), :])).astype(BF16)
                og[o, 1] = (wide(l1r[s]) + wide(dw[q, ds(left * dl + half, half), :])).astype(BF16)
                start(rg_next(u))

            @product
            def add_d(v):
                s = lax.rem(v, RING)
                o = lax.rem(s, HELD)
                take_d(2 * piece, rd_a.at[s])
                take_d(2 * piece, lown.at[0, s])
                od[o, 0] = (wide(k1l[s]) + wide(own[s, pl.ds(0, piece), :])).astype(BF16)
                od[o, 1] = (wide(k1r[s]) + wide(own[s, pl.ds(piece, piece), :])).astype(BF16)
                start(rd_next(v))

            at(tL + 1, 2 * NT, add_g)
            at(tL + 6, 2 * NT, add_d)

            @product
            def back_3(u):
                at_, s = dwd_out(u), lax.rem(u, 2)
                dwd[s] = nn(yT[...], prod[...]).astype(BF16).T
                start(at_)

            at(tL, 2 * NT, back_3)
            at(tL, 2 * NT, lambda u: start(rg_first(u)))

            @product
            def back_4(u):
                s = lax.rem(u + NT, 2)

                def part(m, _):
                    r = ds(m * span, span, span)
                    acc[r, :] += nt(dgu[r, :], wgu_v[s])
                    return 0

                lax.fori_loop(0, tokens // span, part, 0)

            at(tL, NT, back_4)

            @product
            def total_g(u):
                s, q, f = lax.rem(u, RING), lax.rem(u, KEEP), lax.rem(u, 2)
                take_g(4 * half, rg_b.at[s])
                lo = wide(dw[q, ds(me * dl, half), :]) + wide(l3l[s]) + wide(l2r[s])
                hi = wide(dw[q, ds(me * dl + half, half), :]) + wide(l3r[s]) + wide(l2l[s])
                lo, hi = lo.astype(BF16), hi.astype(BF16)
                fg[f, pl.ds(0, half), :] = lo
                fg[f, pl.ds(half, half), :] = hi
                lo, hi = wide(lo), wide(hi)
                sg[...] += jnp.sum((lo * lo + hi * hi).reshape(half // 8, 8, 2 * TILE), 0)
                start(g_out(u))
                take_g(6 * half, rg_s.at[s])

            @product
            def total_d(v):
                s, f = lax.rem(v, RING), lax.rem(v, 2)
                take_d(4 * piece, rd_b.at[s])
                take_d(2 * piece, lown.at[1, s])
                lo = wide(own[s, pl.ds(2 * piece, piece), :]) + wide(k3l[s]) + wide(k2r[s])
                hi = wide(own[s, pl.ds(3 * piece, piece), :]) + wide(k3r[s]) + wide(k2l[s])
                lo, hi = lo.astype(BF16), hi.astype(BF16)
                fd[f, pl.ds(0, piece), :] = lo
                fd[f, pl.ds(piece, piece), :] = hi
                lo, hi = wide(lo), wide(hi)
                sd[...] += jnp.sum((lo * lo + hi * hi).reshape(piece // 8, 8, d), 0)
                start(d_out(v))
                take_d(6 * piece, rd_s.at[s])

            at(tL + 4, 2 * NT, lambda u: take_g(dl, lout.at[0, lax.rem(u, 2)]))
            at(tL + 3, 2 * NT, total_g)
            at(tL + 9, 2 * NT, lambda v: done(d_out(v)))
            at(tL + 8, 2 * NT, total_d)

        for lo_, hi_ in ((0, tF), (tF, tL), (tL, tB), (tB, tE), (tE, end + 1)):

            def step(t, _, lo_=lo_, hi_=hi_):
                loop(t, lo_, hi_)
                return 0

            lax.fori_loop(lo_, hi_, step, 0)

        parts = [sg[:, k * 128 : (k + 1) * 128] for k in range(2 * TILE // 128)] + [sd[:, k * 128 : (k + 1) * 128] for k in range(d // 128)]
        st[3] = sum(parts[1:], parts[0])
        sends = [remote(st.at[3], st.at[k], st_s.at[k], st_r.at[k], to) for k, to in enumerate((R, L, O))]
        start(sends)
        done(sends)
        st[4] = st[0] + st[1] + st[2] + st[3]
        last = [local(st.at[4], stat, lin.at[0])]
        start(last)
        done(last)

    any_ = pl.BlockSpec(memory_space=pl.ANY)
    shapes = [
        ((layers, dl, ff), BF16), ((layers, dl, ff), BF16), ((layers, fl, d), BF16), ((8, 128), F32),
        ((layers, NT, d, 2 * TILE), BF16), ((layers, ff, d), BF16), ((layers, ff, d), BF16),
    ]
    V, S = pltpu.VMEM, pltpu.SemaphoreType.DMA
    scratch = [
        V((layers, tokens, d), BF16), V((layers, d, tokens), BF16), V((tokens, d), BF16), V((d, tokens), BF16), V((tokens, d), BF16),
        V((tokens, d), F32), V((tokens, TILE), BF16), V((tokens, 2 * TILE), BF16),
        V((2, d, 2 * TILE), BF16), V((2, TILE, d), BF16), V((KEEP, d, 2 * TILE), BF16), V((2, TILE, d), BF16),
        V((2, dl, 2 * TILE), BF16), V((2, 2 * piece, d), BF16), V((HELD, 2, half, 2 * TILE), BF16), V((HELD, 2, piece, d), BF16),
        V((RING, 4 * piece, d), BF16),
    ]
    scratch += [V((RING, half, 2 * TILE), BF16)] * 6 + [V((RING, piece, d), BF16)] * 6
    scratch += [V((8, 2 * TILE), F32), V((8, d), F32), V((5, 8, 128), F32)]
    way = [S((NT,)), S((3, TURNS)), S((layers, TURNS)), S((TURNS,))]
    scratch += way + way + [S((RING,))] * 6
    scratch += [S((2,)), S((2, RING)), S((2, 2)), S((2,)), S((3,)), S((3,)), S((3,))]
    return pl.pallas_call(
        body,
        out_shape=[jax.ShapeDtypeStruct(*s) for s in shapes],
        in_specs=[any_] * 5,
        out_specs=[any_] * 7,
        scratch_shapes=scratch,
        compiler_params=pltpu.CompilerParams(collective_id=0, has_side_effects=True, vmem_limit_bytes=67043328),
        name="exchange",
    )


def adamw(n, layers, dl, ff, fl, d):
    count = n * layers * (2 * dl * ff + fl * d)
    steps = 8

    def body(stat, *refs):
        ins, outs = refs[:12], refs[12:]
        factor = jnp.minimum(1.0, 0.5 * lax.rsqrt(jnp.sum(stat[...]) / count + 1e-30))
        for i in range(3):
            g, w, m, v = (ins[4 * i + k] for k in range(4))
            by = g[...].astype(F32) * factor
            first = 0.9 * m[...] + 0.1 * by
            second = 0.95 * v[...] + 0.05 * by * by
            old = w[...].astype(F32)
            outs[i][...] = (old - 0.02 * (first * lax.rsqrt(second + 1e-8) + 0.1 * old)).astype(BF16)
            outs[3 + i][...] = first
            outs[6 + i][...] = second

    sizes = [(layers * dl, ff), (layers * dl, ff), (layers * fl, d)]
    kinds = [pl.BlockSpec((rows // steps, columns), lambda i: (i, 0)) for rows, columns in sizes]
    call = pl.pallas_call(
        body,
        grid=(steps,),
        in_specs=[pl.BlockSpec((8, 128), lambda i: (0, 0))] + [k for k in kinds for _ in range(4)],
        out_specs=kinds * 3,
        out_shape=[jax.ShapeDtypeStruct(s, t) for t in (BF16, F32, F32) for s in sizes],
        compiler_params=pltpu.CompilerParams(vmem_limit_bytes=67043328),
        name="adamw",
    )

    def run(stat, gradients, weights, m, v):
        flat = [one.reshape(-1, one.shape[-1]) for four in zip(gradients, weights, m, v, strict=True) for one in four]
        shapes = [w.shape for w in weights] * 3
        return tuple(out.reshape(s) for out, s in zip(call(stat, *flat), shapes, strict=True))

    return run


def solution(mesh):
    n = mesh.shape["dp"]

    def step(x, dy, *arrays):
        weights, m, v = (arrays[i : i + 3] for i in (0, 3, 6))
        layers, ff, d = weights[2].shape[0], weights[2].shape[1] * n, weights[2].shape[2]
        *gradients, stat = exchange(n, x.shape[1], d, ff, layers)(x[0], dy[0], *weights)[:4]
        return adamw(n, layers, d // n, ff, ff // n, d)(stat, gradients, weights, m, v)

    states, cut = P(("rep", "dp"), None, None), P(None, "dp", None)
    return jax.shard_map(
        step,
        mesh=mesh,
        in_specs=(states, states) + (cut,) * 9,
        out_specs=(P("rep", "dp", None),) * 9,
        check_vma=False,
    )
```

```python
import jax
import jax.numpy as jnp
from jax import lax
from jax.experimental import pallas as pl
from jax.experimental.pallas import tpu as pltpu
from jax.sharding import PartitionSpec as P

F32, BF16 = jnp.float32, jnp.bfloat16
TILE = 256
RING = 8
TURNS = 12
KEEP = 4
HELD = 4


def nn(a, b):
    return lax.dot_general(a, b, (((1,), (0,)), ((), ())), preferred_element_type=F32)


def nt(a, b):
    return lax.dot_general(a, b, (((1,), (1,)), ((), ())), preferred_element_type=F32)


def exchange(n, tokens, d, ff, layers):
    assert n == 4 and layers == 2
    dl, fl, nt_ = d // n, ff // n, ff // TILE
    half, piece = dl // 2, fl // nt_ // 2
    lent = (half * 2 // 7, half // 2)
    lent_d = piece // 2
    rows, span = min(512, tokens), min(1024, tokens)
    begin = 6
    late = 5
    NT = nt_
    m4 = NT - 3
    assert m4 % 4 == 0 and ff == n * NT * 64

    def tile(j):
        return jnp.where(j < m4, (m4 // 4 + 1) * lax.rem(j, 4) + lax.div(j, 4), (m4 // 4 + 1) * (j - m4) + m4 // 4)

    def unit(block, v):
        return jnp.where(v < m4, block + v, jnp.where(v - m4 < block, v - m4, v))

    def body(
        x, dy, wg, wu, wd,
        gg, gu, gd, stat, WGU, WD, DWD,
        a, aT, y, yT, h, acc, prod, dgu, wgu_v, wd_v, dw, dwd, fg, fd, og, od, own,
        l1l, l1r, l2l, l2r, l3l, l3r, k1l, k1r, k2l, k2r, k3l, k3r, sg, sd, st,
        ad_1, ad_n, ad_a, ad_b, ag_1, ag_n, ag_a, ag_b, rg_s, rg_a, rg_b, rd_s, rd_a, rd_b, ld, lown, lout, lst, lin, st_s, st_r,
    ):
        me, rep = lax.axis_index("dp"), lax.axis_index("rep")
        right, left, far = (lax.rem(me + k, n) for k in (1, n - 1, 2))
        core = lax.rem(rep, 2)
        chip = lax.rem(lax.div(rep, 2), 2)
        R, L, O, C, Y = {"dp": right}, {"dp": left}, {"dp": far}, {"rep": rep + 1 - 2 * core}, {"rep": rep + 2 - 4 * chip}

        def remote(src, dst, ss, rs, to):
            return lambda: pltpu.make_async_remote_copy(
                src_ref=src, dst_ref=dst, send_sem=ss, recv_sem=rs, device_id=to, device_id_type=pl.DeviceIdType.MESH
            )

        def local(src, dst, sem):
            return lambda: pltpu.make_async_copy(src, dst, sem)

        def ds(at, size, by=16):
            return pl.ds(pl.multiple_of(at, by), size)

        barrier = pltpu.get_barrier_semaphore()
        for to in (R, L, O, C, Y):
            pl.semaphore_signal(barrier, inc=1, device_id=to, device_id_type=pl.DeviceIdType.MESH)
        pl.semaphore_wait(barrier, 5)

        def take_g(rows_, sem):
            pltpu.make_async_copy(WGU.at[0, 0, pl.ds(0, rows_)], WGU.at[0, 0, pl.ds(0, rows_)], sem).wait()

        def take_d(rows_, sem):
            pltpu.make_async_copy(WD.at[0, pl.ds(0, rows_)], WD.at[0, pl.ds(0, rows_)], sem).wait()

        class Way:
            def __init__(self, take, first, pass_on, share, whole, got, sent_a, sent_b, sizes, soon):
                lo, hi = pass_on
                self.soon = soon
                self.take, self.got, self.sent_a, self.sent_b, self.sizes = take, got, sent_a, sent_b, sizes
                self.first = [remote(src, dst, sent_a, got[0], to) for src, dst, to in first]
                self.second = [remote(lo, lo, sent_b, got[1], R), remote(hi, hi, sent_b, got[1], L)]
                self.across = [remote(share(b), share(b), sent_b, got[2], Y) for b in (left, right, far)] if sizes[2] else []
                self.inside = [remote(whole(b), whole(b), sent_b, got[3], C) for b in (left, right, far)]

            def go(self, step):
                if step and self.sizes[step - 1]:
                    self.take(self.sizes[step - 1], self.got[step - 1])
                k = 2 if self.soon else 0
                start((self.first, self.second + self.across[:k], self.across[k:], self.inside, ())[step])

            def sent_first(self):
                self.take(self.sizes[0], self.sent_a)

            def sent_rest(self):
                self.take(sum(self.sizes[1:]), self.sent_b)

        def d_in(l, j, many, few=lent_d):
            s, few, part = lax.rem(l * (NT + 1) + j, TURNS), many * few, many * piece
            most = part - few

            def rows_of(block, at, size):
                return ds(block * fl + 2 * piece * unit(block, j) + part * core + at, size, 8)

            mine = wd.at[l, ds(2 * piece * unit(me, j) + part * core + chip * few, most)]
            to = WD.at[l, rows_of(me, chip * few, most)]
            lo = WD.at[l, rows_of(left, chip * few, most // 2)]
            hi = WD.at[l, rows_of(right, chip * few + most // 2, most // 2)]
            share = lambda b: WD.at[l, rows_of(b, chip * most, few)]
            whole = lambda b: WD.at[l, rows_of(b, 0, part)]
            got = [ad_1.at[j]] + [ad_n.at[i, s] for i in range(3)]
            sizes = (2 * most, most, 3 * few, 3 * part)
            return Way(take_d, [(mine, to, R), (mine, to, L)], (lo, hi), share, whole, got, ad_a.at[l, lax.rem(j, TURNS)], ad_b.at[s], sizes, l == 0)

        def g_in(l, j):
            s, few = lax.rem(l * NT + j, TURNS), lent[l]
            most = half - few

            def rows_of(block, at, size):
                return ds(block * dl + core * half + at, size, 8)

            first = []
            for k, w in enumerate((wg, wu)):
                src = w.at[l, ds(core * half + chip * few, most, 8), ds(tile(j) * TILE, TILE, TILE)]
                dst = WGU.at[l, j, rows_of(me, chip * few, most), pl.ds(k * TILE, TILE)]
                first += [(src, dst, R), (src, dst, L)]
            lo = WGU.at[l, j, rows_of(left, chip * few, most), pl.ds(0, TILE)]
            hi = WGU.at[l, j, rows_of(right, chip * few, most), pl.ds(TILE, TILE)]
            share = lambda b: WGU.at[l, j, rows_of(b, chip * most, few)]
            whole = lambda b: WGU.at[l, j, rows_of(b, 0, half)]
            got = [ag_1.at[j]] + [ag_n.at[i, s] for i in range(3)]
            sizes = (2 * most, most, 3 * few, 3 * half)
            return Way(take_g, first, (lo, hi), share, whole, got, ag_a.at[l, lax.rem(j, TURNS)], ag_b.at[s], sizes, l == 0)

        def loads(l, j, k):
            s = lax.rem(k, 2)
            out = [
                local(wg.at[l, :, ds(tile(j) * TILE, TILE, TILE)], wgu_v.at[s, ds(me * dl, dl), pl.ds(0, TILE)], ld.at[s]),
                local(wu.at[l, :, ds(tile(j) * TILE, TILE, TILE)], wgu_v.at[s, ds(me * dl, dl), pl.ds(TILE, TILE)], ld.at[s]),
                local(WD.at[l, ds(tile(j) * TILE, TILE)], wd_v.at[s], ld.at[s]),
            ]
            for block in (right, left, far):
                at = ds(block * dl, dl)
                out.append(local(WGU.at[l, j, at], wgu_v.at[s, at], ld.at[s]))
            return out

        def loaded(k):
            take_d(3 * TILE, ld.at[lax.rem(k, 2)])

        def sum_first(src, slot, land, ss, ra, rb):
            return [
                remote(src(far, 0), land[0].at[slot], ss.at[slot], ra.at[slot], R),
                remote(src(far, 1), land[1].at[slot], ss.at[slot], ra.at[slot], L),
                remote(src(right, 1), land[2].at[slot], ss.at[slot], rb.at[slot], R),
                remote(src(left, 0), land[3].at[slot], ss.at[slot], rb.at[slot], L),
            ]

        def sum_next(out, slot, land, ss, rb):
            return [
                remote(out.at[lax.rem(slot, HELD), 0], land[4].at[slot], ss.at[slot], rb.at[slot], R),
                remote(out.at[lax.rem(slot, HELD), 1], land[5].at[slot], ss.at[slot], rb.at[slot], L),
            ]

        land_g, land_d = (l1l, l1r, l2l, l2r, l3l, l3r), (k1l, k1r, k2l, k2r, k3l, k3r)

        def rg_first(u):
            q = lax.rem(u, KEEP)
            return sum_first(lambda b, k: dw.at[q, ds(b * dl + k * half, half)], lax.rem(u, RING), land_g, rg_s, rg_a, rg_b)

        def rg_next(u):
            return sum_next(og, lax.rem(u, RING), land_g, rg_s, rg_b)

        def rd_first(v):
            l, j = 1 - lax.div(v, NT), lax.rem(v, NT)
            at = lambda b, k: DWD.at[l, ds(b * fl + (2 * unit(b, j) + k) * piece, piece)]
            return sum_first(at, lax.rem(v, RING), land_d, rd_s, rd_a, rd_b)

        def rd_next(v):
            return sum_next(od, lax.rem(v, RING), land_d, rd_s, rd_b)

        def own_loads(v):
            l, j, s = 1 - lax.div(v, NT), lax.rem(v, NT), lax.rem(v, RING)
            at = lambda b, k, m: DWD.at[l, ds(b * fl + (2 * unit(b, j) + k) * piece, m * piece)]
            return [
                local(at(right, 0, 1), own.at[s, pl.ds(0, piece)], lown.at[0, s]),
                local(at(left, 1, 1), own.at[s, pl.ds(piece, piece)], lown.at[0, s]),
                local(at(me, 0, 2), own.at[s, pl.ds(2 * piece, 2 * piece)], lown.at[1, s]),
            ]

        def g_out(u):
            l, j, s = 1 - lax.div(u, NT), lax.rem(u, NT), lax.rem(u, 2)
            to = ds(tile(j) * TILE, TILE, TILE)
            return [
                local(fg.at[s, :, pl.ds(0, TILE)], gg.at[l, :, to], lout.at[0, s]),
                local(fg.at[s, :, pl.ds(TILE, TILE)], gu.at[l, :, to], lout.at[0, s]),
            ]

        def d_out(v):
            l, j, s = 1 - lax.div(v, NT), lax.rem(v, NT), lax.rem(v, 2)
            return [local(fd.at[s], gd.at[l, ds(unit(me, j) * 2 * piece, 2 * piece)], lout.at[1, s])]

        def dwd_out(u):
            l, j, s = 1 - lax.div(u, NT), lax.rem(u, NT), lax.rem(u, 2)
            return [local(dwd.at[s], DWD.at[l, ds(tile(j) * TILE, TILE)], lst.at[s])]

        def start(copies):
            for c in copies:
                c().start()

        def done(copies):
            for c in copies:
                c().wait()

        def wide(ref):
            return ref.astype(F32)

        tF = 7
        tL, tB, tE = tF + NT, tF + 2 * NT, tF + 3 * NT
        end = tE + 8
        blk = min(256, tokens)
        nblk = tokens // blk

        aside = a.at[1, pl.ds(0, fl)]
        own_w = [[local(wd.at[l], aside, lin.at[0])] for l in range(layers)]
        put_w = [[local(aside, WD.at[l, ds(me * fl, fl)], lin.at[0])] for l in range(layers)]
        own_x = [local(x, h, lin.at[1]), local(dy, y, lin.at[2])]

        def norm_into(l, r):
            hw = wide(h[r, :])
            scale = lax.rsqrt(jnp.mean(hw * hw, -1, keepdims=True) + 1e-6)
            n_ = (hw * scale).astype(BF16)
            a[l, r, :] = n_
            aT[l, :, r] = n_.T

        def loop(t, lo_, hi_):
            def when(*terms, within=(0, end + 1)):
                if within[0] >= hi_ or within[1] <= lo_:
                    return lambda f: None
                if within[0] <= lo_ and within[1] >= hi_ and not terms:
                    return lambda f: f()
                test = (t >= within[0]) & (t < within[1])
                for term in terms:
                    test = test & term
                return pl.when(test)

            def at(t0, count, f):
                when(*([t >= 0] if f in products else []), within=(t0, t0 + count))(lambda: f(t - t0))

            products = []

            def product(f):
                products.append(f)
                return f

            def once(t0):
                return when(within=(t0, t0 + 1))

            def ramp(ahead, more, f, late=0):
                lo, hi = (
                    jnp.clip(s - tF + ahead + jnp.clip(s - tF - late, 0, more) - jnp.where((s == tF) & (late == 3), 1, 0), 0, NT) for s in (t, t + 1)
                )

                when(hi > lo + 1, within=(tF - ahead, tL))(lambda: f(lo))
                when(hi > lo, within=(tF - ahead, tL))(lambda: f(hi - 1))

            def at4(l, first, then, f, only=None):
                if only != "then":
                    once(first)(lambda: f(d_in(l, 0, 4, 0)))
                if only != "first":
                    k = t - then
                    when(lax.rem(k, 4) == 0, within=(then + 1, then + m4))(lambda: f(d_in(l, k, 4)))

                    @once(then + m4)
                    def _():
                        def one(v, _):
                            f(d_in(l, v, 1))
                            return 0

                        lax.fori_loop(m4, NT, one, 0)

            at(tF - 4, NT, lambda j: g_in(0, j).sent_first())
            at4(0, tF - 4, tF - 4, lambda w: w.sent_first())
            for l in range(layers):
                at(tF + l * NT + 1, NT, lambda j: g_in(l, j).sent_rest())
                at4(l, tF + l * NT, tF + l * NT, lambda w: w.sent_rest())
            at4(0, tF - 7, tF - 8, lambda w: w.go(0))
            ramp(6, 4, lambda j: g_in(0, j).go(0))

            at(tF + begin + 4, NT - late, lambda j: g_in(1, j).sent_first())
            at(tL + 4, late, lambda j: g_in(1, NT - late + j).sent_first())
            at4(1, tF + begin + 4, tF + begin + 4, lambda w: w.sent_first())
            at(tF + begin, NT - late, lambda j: g_in(1, j).go(0))
            at4(1, tF + begin, tF + begin, lambda w: w.go(0))

            @once(tL)
            def _():
                def one(j, _):
                    g_in(1, j).go(0)
                    return 0

                lax.fori_loop(NT - late, NT, one, 0)

            at(tL + 1, 2 * NT, lambda u: done(dwd_out(u)))
            at(tL + 4, 2 * NT, lambda v: start(rd_first(v) + own_loads(v)))

            @once(0)
            def _():
                start(own_x + own_w[0])
                acc[...] = jnp.zeros_like(acc)
                sg[...] = jnp.zeros_like(sg)
                sd[...] = jnp.zeros_like(sd)

            @once(1)
            def _():
                done(own_x)

                def start_on(m, _):
                    r = ds(m * blk, blk, blk)
                    norm_into(0, r)
                    yT[:, r] = y[r, :].T
                    return 0

                lax.fori_loop(0, nblk, start_on, 0)
                done(own_w[0])
                start(put_w[0])

            @once(2)
            def _():
                done(put_w[0])
                start(own_w[1])

            @once(3)
            def _():
                done(own_w[1])
                start(put_w[1])

            @once(4)
            def _():
                done(put_w[1])

            @once(tL)
            def _():
                def piece_(m, _):
                    r = ds(m * blk, blk, blk)
                    h[r, :] = (wide(h[r, :]) + wide(acc[r, :].astype(BF16))).astype(BF16)
                    norm_into(1, r)
                    return 0

                lax.fori_loop(0, nblk, piece_, 0)

            @once(tB)
            def _():
                def piece_(m, _):
                    r = ds(m * blk, blk, blk)
                    hw, da = wide(h[r, :]), wide(acc[r, :].astype(BF16))
                    scale = lax.rsqrt(jnp.mean(hw * hw, -1, keepdims=True) + 1e-6)
                    by_scale = jnp.sum(da * hw, -1, keepdims=True)
                    by_h = (da * scale - hw * (by_scale * scale * scale * scale * (1.0 / d))).astype(BF16)
                    by = (wide(y[r, :]) + wide(by_h)).astype(BF16)
                    y[r, :] = by
                    yT[:, r] = by.T
                    return 0

                lax.fori_loop(0, nblk, piece_, 0)

            for l in range(layers):
                at(tF + l * NT - 1, NT, lambda j: g_in(l, j).go(4))

            for l in range(layers):
                at4(l, tF + l * NT - 1, tF + l * NT - 1, lambda w: w.go(4))

            k = t + 1 - tF

            @when(within=(tF - 1, tE - 1))
            def _():
                start(loads(lax.rem(lax.div(k, NT), 2), lax.rem(k, NT), k))

            @product
            def forward(j):
                s = lax.rem(j, 2)
                loaded(j)

                for m in range(tokens // span):
                    r = pl.ds(m * span, span)
                    both = nn(a[0, r, :], wgu_v[s])
                    gate, up = both[:, :TILE], both[:, TILE:]
                    p = (gate * (1 / (1 + jnp.exp(-gate))) * up).astype(BF16)
                    acc[r, :] += nn(p, wd_v[s])

            at(tF, NT, forward)

            @product
            def back_1(u):
                l, s = 1 - lax.div(u, NT), lax.rem(u + NT, 2)
                loaded(u + NT)

                for m in range(tokens // rows):
                    r = pl.ds(m * rows, rows)
                    both = nn(a[l, r, :], wgu_v[s])
                    gate, up = both[:, :TILE], both[:, TILE:]
                    by = wide(nt(y[r, :], wd_v[s]).astype(BF16))
                    sig = 1 / (1 + jnp.exp(-gate))
                    act = gate * sig
                    prod[r, :] = (act * up).astype(BF16)
                    dgu[r, TILE:] = (by * act).astype(BF16)
                    dgu[r, :TILE] = (by * up * (sig * (1 + gate * (1 - sig)))).astype(BF16)

            at(tL, 2 * NT, back_1)

            for k, ahead, more, ahead_0, ahead_d, ahead_1 in ((3, 3, 1, 3, 3, 2), (2, 4, 2, 3, 4, 4), (1, 5, 3, 5, 6, 8)):
                ramp(ahead, more, lambda j: g_in(0, j).go(k), k)
                at4(0, tF - ahead_0, tF - ahead_d, lambda w: w.go(k), "then" if k == 3 else None)
                if k == 2:
                    at4(0, tF - ahead_0, tF - ahead_d, lambda w: w.go(3), "first")
                at(tL - ahead_1, NT, lambda j: g_in(1, j).go(k))
                at4(1, tL - ahead_1, tL - ahead_1, lambda w: w.go(k))

            @product
            def back_2(u):
                l, q = 1 - lax.div(u, NT), lax.rem(u, KEEP)

                dw[q] = nn(aT[l], dgu[...]).astype(BF16)

            at(tL, 2 * NT, back_2)

            @product
            def add_g(u):
                s, q = lax.rem(u, RING), lax.rem(u, KEEP)
                o = lax.rem(s, HELD)
                take_g(2 * half, rg_a.at[s])
                og[o, 0] = (wide(l1l[s]) + wide(dw[q, ds(right * dl, half), :])).astype(BF16)
                og[o, 1] = (wide(l1r[s]) + wide(dw[q, ds(left * dl + half, half), :])).astype(BF16)
                start(rg_next(u))

            @product
            def add_d(v):
                s = lax.rem(v, RING)
                o = lax.rem(s, HELD)
                take_d(2 * piece, rd_a.at[s])
                take_d(2 * piece, lown.at[0, s])
                od[o, 0] = (wide(k1l[s]) + wide(own[s, pl.ds(0, piece), :])).astype(BF16)
                od[o, 1] = (wide(k1r[s]) + wide(own[s, pl.ds(piece, piece), :])).astype(BF16)
                start(rd_next(v))

            at(tL + 1, 2 * NT, add_g)
            at(tL + 6, 2 * NT, add_d)

            @product
            def back_3(u):
                at_, s = dwd_out(u), lax.rem(u, 2)
                dwd[s] = nn(yT[...], prod[...]).astype(BF16).T
                start(at_)

            at(tL, 2 * NT, back_3)
            at(tL, 2 * NT, lambda u: start(rg_first(u)))

            @product
            def back_4(u):
                s = lax.rem(u + NT, 2)

                def part(m, _):
                    r = ds(m * span, span, span)
                    acc[r, :] = nt(dgu[r, :], wgu_v[s]) + jnp.where(u > 0, acc[r, :], 0.0)
                    return 0

                lax.fori_loop(0, tokens // span, part, 0)

            at(tL, NT, back_4)

            @product
            def total_g(u):
                s, q, f = lax.rem(u, RING), lax.rem(u, KEEP), lax.rem(u, 2)
                take_g(4 * half, rg_b.at[s])
                lo = wide(dw[q, ds(me * dl, half), :]) + wide(l3l[s]) + wide(l2r[s])
                hi = wide(dw[q, ds(me * dl + half, half), :]) + wide(l3r[s]) + wide(l2l[s])
                lo, hi = lo.astype(BF16), hi.astype(BF16)
                fg[f, pl.ds(0, half), :] = lo
                fg[f, pl.ds(half, half), :] = hi
                lo, hi = wide(lo), wide(hi)
                sg[...] += jnp.sum((lo * lo + hi * hi).reshape(half // 8, 8, 2 * TILE), 0)
                start(g_out(u))
                take_g(6 * half, rg_s.at[s])

            @product
            def total_d(v):
                s, f = lax.rem(v, RING), lax.rem(v, 2)
                take_d(4 * piece, rd_b.at[s])
                take_d(2 * piece, lown.at[1, s])
                lo = wide(own[s, pl.ds(2 * piece, piece), :]) + wide(k3l[s]) + wide(k2r[s])
                hi = wide(own[s, pl.ds(3 * piece, piece), :]) + wide(k3r[s]) + wide(k2l[s])
                lo, hi = lo.astype(BF16), hi.astype(BF16)
                fd[f, pl.ds(0, piece), :] = lo
                fd[f, pl.ds(piece, piece), :] = hi
                lo, hi = wide(lo), wide(hi)
                sd[...] += jnp.sum((lo * lo + hi * hi).reshape(piece // 8, 8, d), 0)
                start(d_out(v))
                take_d(6 * piece, rd_s.at[s])

            at(tL + 4, 2 * NT, lambda u: take_g(dl, lout.at[0, lax.rem(u, 2)]))
            at(tL + 3, 2 * NT, total_g)
            at(tL + 9, 2 * NT, lambda v: done(d_out(v)))
            at(tL + 8, 2 * NT, total_d)

        for lo_, hi_ in ((0, tF), (tF, tL), (tL, tB), (tB, tE), (tE, end + 1)):

            def step(t, _, lo_=lo_, hi_=hi_):
                loop(t, lo_, hi_)
                return 0

            lax.fori_loop(lo_, hi_, step, 0)

        parts = [sg[:, k * 128 : (k + 1) * 128] for k in range(2 * TILE // 128)] + [sd[:, k * 128 : (k + 1) * 128] for k in range(d // 128)]
        st[3] = sum(parts[1:], parts[0])
        sends = [remote(st.at[3], st.at[k], st_s.at[k], st_r.at[k], to) for k, to in enumerate((R, L, O))]
        start(sends)
        done(sends)
        st[4] = st[0] + st[1] + st[2] + st[3]
        last = [local(st.at[4], stat, lin.at[0])]
        start(last)
        done(last)

    any_ = pl.BlockSpec(memory_space=pl.ANY)
    shapes = [
        ((layers, dl, ff), BF16), ((layers, dl, ff), BF16), ((layers, fl, d), BF16), ((8, 128), F32),
        ((layers, NT, d, 2 * TILE), BF16), ((layers, ff, d), BF16), ((layers, ff, d), BF16),
    ]
    V, S = pltpu.VMEM, pltpu.SemaphoreType.DMA
    scratch = [
        V((layers, tokens, d), BF16), V((layers, d, tokens), BF16), V((tokens, d), BF16), V((d, tokens), BF16), V((tokens, d), BF16),
        V((tokens, d), F32), V((tokens, TILE), BF16), V((tokens, 2 * TILE), BF16),
        V((2, d, 2 * TILE), BF16), V((2, TILE, d), BF16), V((KEEP, d, 2 * TILE), BF16), V((2, TILE, d), BF16),
        V((2, dl, 2 * TILE), BF16), V((2, 2 * piece, d), BF16), V((HELD, 2, half, 2 * TILE), BF16), V((HELD, 2, piece, d), BF16),
        V((RING, 4 * piece, d), BF16),
    ]
    scratch += [V((RING, half, 2 * TILE), BF16)] * 6 + [V((RING, piece, d), BF16)] * 6
    scratch += [V((8, 2 * TILE), F32), V((8, d), F32), V((5, 8, 128), F32)]
    way = [S((NT,)), S((3, TURNS)), S((layers, TURNS)), S((TURNS,))]
    scratch += way + way + [S((RING,))] * 6
    scratch += [S((2,)), S((2, RING)), S((2, 2)), S((2,)), S((3,)), S((3,)), S((3,))]
    return pl.pallas_call(
        body,
        out_shape=[jax.ShapeDtypeStruct(*s) for s in shapes],
        in_specs=[any_] * 5,
        out_specs=[any_] * 7,
        scratch_shapes=scratch,
        compiler_params=pltpu.CompilerParams(collective_id=0, has_side_effects=True, vmem_limit_bytes=67043328),
        name="exchange",
    )


def adamw(n, layers, dl, ff, fl, d):
    count = n * layers * (2 * dl * ff + fl * d)
    steps = 8

    def body(stat, *refs):
        ins, outs = refs[:12], refs[12:]
        factor = jnp.minimum(1.0, 0.5 * lax.rsqrt(jnp.sum(stat[...]) / count + 1e-30))
        for i in range(3):
            g, w, m, v = (ins[4 * i + k] for k in range(4))
            by = g[...].astype(F32) * factor
            first = 0.9 * m[...] + 0.1 * by
            second = 0.95 * v[...] + 0.05 * by * by
            old = w[...].astype(F32)
            outs[i][...] = (old - 0.02 * (first * lax.rsqrt(second + 1e-8) + 0.1 * old)).astype(BF16)
            outs[3 + i][...] = first
            outs[6 + i][...] = second

    sizes = [(layers * dl, ff), (layers * dl, ff), (layers * fl, d)]
    kinds = [pl.BlockSpec((rows // steps, columns), lambda i: (i, 0)) for rows, columns in sizes]
    call = pl.pallas_call(
        body,
        grid=(steps,),
        in_specs=[pl.BlockSpec((8, 128), lambda i: (0, 0))] + [k for k in kinds for _ in range(4)],
        out_specs=kinds * 3,
        out_shape=[jax.ShapeDtypeStruct(s, t) for t in (BF16, F32, F32) for s in sizes],
        compiler_params=pltpu.CompilerParams(vmem_limit_bytes=67043328),
        name="adamw",
    )

    def run(stat, gradients, weights, m, v):
        flat = [one.reshape(-1, one.shape[-1]) for four in zip(gradients, weights, m, v, strict=True) for one in four]
        shapes = [w.shape for w in weights] * 3
        return tuple(out.reshape(s) for out, s in zip(call(stat, *flat), shapes, strict=True))

    return run


def solution(mesh):
    n = mesh.shape["dp"]

    def step(x, dy, *arrays):
        weights, m, v = (arrays[i : i + 3] for i in (0, 3, 6))
        layers, ff, d = weights[2].shape[0], weights[2].shape[1] * n, weights[2].shape[2]
        *gradients, stat = exchange(n, x.shape[1], d, ff, layers)(x[0], dy[0], *weights)[:4]
        return adamw(n, layers, d // n, ff, ff // n, d)(stat, gradients, weights, m, v)

    states, cut = P(("rep", "dp"), None, None), P(None, "dp", None)
    return jax.shard_map(
        step,
        mesh=mesh,
        in_specs=(states, states) + (cut,) * 9,
        out_specs=(P("rep", "dp", None),) * 9,
        check_vma=False,
    )
```
